32 devices in a mesh: dp: 2 (over x), y: 4 (over z), x: 4 (over y, core).
Axes of the slice: x: 2, y: 2, z: 4, core: 2. Of those that a mesh axis runs over, the one named last changes fastest.
Arguments:
- tokens: int32 [3, 128], P(None, 'dp'), parts along dimension 1
- lengths: int32 [128], P('dp'), parts along dimension 0
- choices: int32 [3, 128, 2], P(None, 'dp'), parts along dimension 1
- emb_table: bfloat16 [122753, 2304], P(None, 'x')
- k_cache: bfloat16 [128, 128, 36, 64], P('dp', None, 'y'), parts along dimension 0
- v_cache: bfloat16 [128, 128, 36, 64], P('dp', None, 'y'), parts along dimension 0
- g_attn: bfloat16 [2304], P('x')
- w_q: bfloat16 [2304, 2304], P('x', 'y')
- w_k: bfloat16 [2304, 2304], P('x', 'y')
- w_v: bfloat16 [2304, 2304], P('x', 'y')
- w_o: bfloat16 [2304, 2304], P('y', 'x')
- g_ffn: bfloat16 [2304], P('x')
- w_router: bfloat16 [2304, 8], P('x')
- w_act: bfloat16 [8, 2304, 5760], P(None, 'x', 'y')
- w_lin: bfloat16 [8, 2304, 5760], P(None, 'x', 'y')
- w_down: bfloat16 [8, 5760, 2304], P(None, 'y', 'x')
Outputs:
- output 1: bfloat16 [3, 128, 2304], P(None, 'dp', 'x'), parts along dimension 1
- output 2: bfloat16 [128, 128, 36, 64], P('dp', None, 'y'), parts along dimension 0
- output 3: bfloat16 [128, 128, 36, 64], P('dp', None, 'y'), parts along dimension 0
There are 2 independent parts. The reference program is written for one: setup_inputs(seed, part) draws one part's arguments, and reference() takes and returns one part's arrays. A program takes and returns all parts, laid end to end along the dimension named above; an argument that names none is the same for every part.
All inputs are finite; a program needn't handle non-finite values.
Results may differ from the reference program's by a relative error of at most 0.0130543.
Values are sent between devices in bfloat16 or wider.
A program may use at most 1 GiB of HBM per device.

```python
import math
import jax
import jax.numpy as jnp
from jax import lax

BATCH = 64
SEQ = 128
D = 2304
HEADS = 36
KV_HEADS = 36
HEAD = 64
FF = 5760
EXPERTS = 8
TOP = 2
VOCAB = 122753
STEPS = 3

EPS = 1e-5
ROPE_BASE = 1.0e6
LOG_SEQ = int(math.log2(SEQ))
HOT_COUNT = max(1, EXPERTS // 8)
GROUP_SIZE = HEADS // KV_HEADS


def draw_lengths(key_a, key_b, key_c):
    exponent = jax.random.randint(key_a, (BATCH,), 0, LOG_SEQ + 1)
    len_limit = jnp.minimum(jnp.left_shift(jnp.ones((BATCH,), jnp.int32), exponent), SEQ - 3)
    raw_draw = jax.random.randint(key_b, (BATCH,), 0, 1 << 30)
    lengths = 1 + raw_draw % len_limit
    pick_row = jax.random.randint(key_c, (), 0, BATCH)
    row_ids = jnp.arange(BATCH)
    lengths = jnp.where(row_ids == pick_row, SEQ - 3, lengths)
    lengths = jnp.where(row_ids == (pick_row + 1) % BATCH, 1, lengths)
    return lengths.astype(jnp.int32)


def draw_choices(key_a, key_b):
    expert_rank = jax.random.permutation(key_a, EXPERTS)
    hot_bonus = jnp.where(expert_rank < HOT_COUNT, EXPERTS, 0)
    noise_int = jax.random.randint(key_b, (STEPS, BATCH, EXPERTS), 0, 2 * EXPERTS)
    scores = (noise_int + hot_bonus) * EXPERTS + jnp.arange(EXPERTS)
    return lax.top_k(scores, TOP)[1].astype(jnp.int32)


def normal_weights(key_w, shape_w, scale_w):
    return (jax.random.normal(key_w, shape_w, jnp.float32) * scale_w).astype(jnp.bfloat16)


def setup_inputs(seed: int = 0, part: int = 0) -> dict:
    base_key = jax.random.key(seed)
    weight_keys = jax.random.split(base_key, 12)
    part_keys = jax.random.split(jax.random.fold_in(base_key, part), 8)
    tokens = jax.random.randint(part_keys[0], (STEPS, BATCH), 0, VOCAB)
    lengths = draw_lengths(part_keys[1], part_keys[2], part_keys[3])
    choices = draw_choices(part_keys[4], part_keys[5])
    k_cache = normal_weights(part_keys[6], (BATCH, SEQ, KV_HEADS, HEAD), 1.0)
    v_cache = normal_weights(part_keys[7], (BATCH, SEQ, KV_HEADS, HEAD), 1.0)
    ramp_rate = jax.random.uniform(weight_keys[0], (), jnp.float32, 0.6, 1.2)
    col_scale = jnp.exp(ramp_rate * jnp.linspace(-1.0, 1.0, D))
    emb_table = (jax.random.normal(weight_keys[1], (VOCAB, D), jnp.float32) * col_scale).astype(jnp.bfloat16)
    g_attn = (1.0 + 0.3 * jax.random.normal(weight_keys[2], (D,), jnp.float32)).astype(jnp.bfloat16)
    w_q = normal_weights(weight_keys[3], (D, HEADS * HEAD), D ** -0.5)
    w_k = normal_weights(weight_keys[4], (D, KV_HEADS * HEAD), D ** -0.5)
    w_v = normal_weights(weight_keys[5], (D, KV_HEADS * HEAD), D ** -0.5)
    w_o = normal_weights(weight_keys[6], (HEADS * HEAD, D), (HEADS * HEAD) ** -0.5)
    g_ffn = (1.0 + 0.3 * jax.random.normal(weight_keys[7], (D,), jnp.float32)).astype(jnp.bfloat16)
    w_router = normal_weights(weight_keys[8], (D, EXPERTS), 1.5 * D ** -0.5)
    w_act = normal_weights(weight_keys[9], (EXPERTS, D, FF), D ** -0.5)
    w_lin = normal_weights(weight_keys[10], (EXPERTS, D, FF), D ** -0.5)
    w_down = normal_weights(weight_keys[11], (EXPERTS, FF, D), FF ** -0.5)
    return dict(tokens=tokens, lengths=lengths, choices=choices, emb_table=emb_table, k_cache=k_cache, v_cache=v_cache, g_attn=g_attn, w_q=w_q, w_k=w_k, w_v=w_v, w_o=w_o, g_ffn=g_ffn, w_router=w_router, w_act=w_act, w_lin=w_lin, w_down=w_down)


def rms_norm(x_val, gain_vec):
    x_f32 = x_val.astype(jnp.float32)
    meansq = jnp.sum(x_f32 * x_f32, axis=-1, keepdims=True) / D
    return (x_f32 * lax.rsqrt(meansq + EPS) * gain_vec.astype(jnp.float32)).astype(jnp.bfloat16)


def rotate(vectors, positions):
    half_dim = HEAD // 2
    inv_freq = ROPE_BASE ** (-(jnp.arange(half_dim).astype(jnp.float32) * 2.0 / HEAD))
    angles = positions.astype(jnp.float32)[:, None, None] * inv_freq
    cosine = jnp.cos(angles)
    sine_val = jnp.sin(angles)
    first_half = vectors[..., :half_dim].astype(jnp.float32)
    second_half = vectors[..., half_dim:].astype(jnp.float32)
    return jnp.concatenate([first_half * cosine - second_half * sine_val, second_half * cosine + first_half * sine_val], axis=-1).astype(jnp.bfloat16)


def attend_row(row_args):
    q_row, key_row, val_row, pos_row = row_args
    scores = jnp.einsum('kgh,skh->kgs', q_row.astype(jnp.float32), key_row.astype(jnp.float32)) * HEAD ** -0.5
    valid_mask = jnp.arange(SEQ) <= pos_row
    scores = jnp.where(valid_mask, scores, -1.0e30)
    peak_val = jnp.max(scores, axis=-1, keepdims=True)
    weight = jnp.where(valid_mask, jnp.exp(scores - peak_val), 0.0)
    total_w = jnp.sum(weight, axis=-1, keepdims=True)
    mixed_out = jnp.einsum('kgs,skh->kgh', weight.astype(jnp.bfloat16).astype(jnp.float32), val_row.astype(jnp.float32))
    return (mixed_out / total_w).astype(jnp.bfloat16)


def reference(tokens, lengths, choices, emb_table, k_cache, v_cache, g_attn, w_q, w_k, w_v, w_o, g_ffn, w_router, w_act, w_lin, w_down):
    slot_ids = jnp.arange(SEQ)
    expert_ids = jnp.arange(EXPERTS)

    def one_step(carry, step_in):
        key_cache, val_cache = carry
        tok_row, choice_row, step_idx = step_in
        positions = lengths + step_idx
        x_in = emb_table[tok_row]
        normed = rms_norm(x_in, g_attn)
        queries = rotate(jnp.dot(normed, w_q, preferred_element_type=jnp.float32).astype(jnp.bfloat16).reshape(BATCH, HEADS, HEAD), positions)
        new_keys = rotate(jnp.dot(normed, w_k, preferred_element_type=jnp.float32).astype(jnp.bfloat16).reshape(BATCH, KV_HEADS, HEAD), positions)
        new_vals = jnp.dot(normed, w_v, preferred_element_type=jnp.float32).astype(jnp.bfloat16).reshape(BATCH, KV_HEADS, HEAD)
        hit_mask = (slot_ids[None, :] == positions[:, None])[:, :, None, None]
        key_cache = jnp.where(hit_mask, new_keys[:, None], key_cache)
        val_cache = jnp.where(hit_mask, new_vals[:, None], val_cache)
        grouped = queries.reshape(BATCH, KV_HEADS, GROUP_SIZE, HEAD)
        mixed = lax.map(attend_row, (grouped, key_cache, val_cache, positions)).reshape(BATCH, HEADS * HEAD)
        x_mid = (x_in.astype(jnp.float32) + jnp.dot(mixed, w_o, preferred_element_type=jnp.float32)).astype(jnp.bfloat16)
        normed2 = rms_norm(x_mid, g_ffn)
        logits = jnp.dot(normed2, w_router, preferred_element_type=jnp.float32)
        gate_val = jax.nn.softmax(jnp.take_along_axis(logits, choice_row, axis=1), axis=-1)
        onehot = choice_row[:, :, None] == expert_ids[None, None, :]
        coef = jnp.sum(jnp.where(onehot, gate_val[:, :, None], 0.0), axis=1)

        def expert_out(expert_args):
            act_w, lin_w, down_w, coef_col = expert_args
            act_f32 = jnp.dot(normed2, act_w, preferred_element_type=jnp.float32)
            lin_f32 = jnp.dot(normed2, lin_w, preferred_element_type=jnp.float32)
            unit_bf16 = (coef_col[:, None] * jax.nn.silu(act_f32) * lin_f32).astype(jnp.bfloat16)
            return jnp.dot(unit_bf16, down_w, preferred_element_type=jnp.float32)

        moe_sum = jnp.sum(lax.map(expert_out, (w_act, w_lin, w_down, coef.T)), axis=0)
        hidden_out = (x_mid.astype(jnp.float32) + moe_sum).astype(jnp.bfloat16)
        return (key_cache, val_cache), hidden_out

    (k_out, v_out), hidden_out = lax.scan(one_step, (k_cache, v_cache), (tokens, choices, jnp.arange(STEPS)))
    return hidden_out, k_out, v_out
```

```python
import functools

import jax
import jax.numpy as jnp
from jax import lax
from jax.experimental import pallas as pl
from jax.experimental.pallas import tpu as pltpu
from jax.sharding import PartitionSpec as P

EPS = 1e-5
ROPE_BASE = 1.0e6
F32 = jnp.float32
BF16 = jnp.bfloat16


def dot(a, b):
    return lax.dot_general(a, b, (((1,), (0,)), ((), ())), preferred_element_type=F32)


def dot_nt(a, b):
    return lax.dot_general(a, b, (((1,), (1,)), ((), ())), preferred_element_type=F32)


def attention_kernel(steps, batch, block, heads, head, lens_ref, qkv_ref, cos_ref, sin_ref, swap_ref, k_in, v_in, o_ref, k_out, v_out, q_rows, kt_ref, vt_ref, o_rows):
    cols = heads * head
    slots = k_in.shape[-1]
    rows = steps * batch
    i = pl.program_id(0)
    hpad = 16

    @pl.when(i == 0)
    def _():
        cosine, sine = cos_ref[...], sin_ref[...]
        for part in range(2):
            val = qkv_ref[:, part * cols:(part + 1) * cols]
            swapped = dot(val, swap_ref[...])
            rot = (val.astype(F32) * cosine + swapped * sine).astype(BF16).astype(F32)
            if part == 0:
                q_rows[...] = rot.reshape(steps, batch, cols)
            else:
                kt_ref[...] = rot.T.astype(BF16)
        vt_ref[...] = qkv_ref[:, 2 * cols:].astype(F32).T.astype(BF16)

    pair = 2
    row_id = lax.broadcasted_iota(jnp.int32, (rows, pair * slots), 0)
    lane_id = lax.broadcasted_iota(jnp.int32, (rows, pair * slots), 1)
    row_t, row_b = row_id // batch, row_id % batch
    lane_s, lane_j = lane_id % slots, lane_id // slots
    head_mask = lax.broadcasted_iota(jnp.int32, (hpad, cols), 1) // head == lax.broadcasted_iota(jnp.int32, (hpad, cols), 0)
    t_of = lax.broadcasted_iota(jnp.int32, (steps * hpad, slots), 0) // hpad
    s_of = lax.broadcasted_iota(jnp.int32, (steps * hpad, slots), 1)
    slot_id = lax.broadcasted_iota(jnp.int32, (cols, slots), 1)

    for p in range(block // pair):
        b0 = i * block + p * pair
        len0, len1 = lens_ref[b0], lens_ref[b0 + 1]
        length = jnp.where(lane_j == 0, len0, len1)
        hot = jnp.where((row_b == b0 + lane_j) & (lane_s == length + row_t), 1.0, 0.0).astype(BF16)
        k_patch = dot(kt_ref[...], hot).astype(BF16)
        v_patch = dot(vt_ref[...], hot).astype(BF16)
        for j in range(pair):
            n = p * pair + j
            b = b0 + j
            first = len0 if j == 0 else len1
            fresh = (slot_id >= first) & (slot_id < first + steps)
            k_new = jnp.where(fresh, k_patch[:, j * slots:(j + 1) * slots], k_in[n].reshape(cols, slots))
            v_new = jnp.where(fresh, v_patch[:, j * slots:(j + 1) * slots], v_in[n].reshape(cols, slots))
            k_out[n] = k_new.reshape(heads, head, slots)
            v_out[n] = v_new.reshape(heads, head, slots)
            q_blk = jnp.concatenate([jnp.where(head_mask, jnp.broadcast_to(q_rows[t, pl.ds(b, 1), :], (hpad, cols)), 0.0) for t in range(steps)], axis=0).astype(BF16)
            scores = dot(q_blk, k_new) * head ** -0.5
            valid = s_of <= first + t_of
            scores = jnp.where(valid, scores, -1.0e30)
            peak = jnp.max(scores, axis=-1, keepdims=True)
            weight = jnp.where(valid, jnp.exp(scores - peak), 0.0)
            total = jnp.sum(weight, axis=-1, keepdims=True)
            mixed = dot_nt(weight.astype(BF16), v_new) / total
            for t in range(steps):
                o_rows[t, pl.ds(b, 1), :] = jnp.sum(jnp.where(head_mask, mixed[t * hpad:(t + 1) * hpad], 0.0), axis=0, keepdims=True)

    @pl.when(i == pl.num_programs(0) - 1)
    def _():
        o_ref[...] = o_rows[...].reshape(rows, cols).astype(BF16)


def attention(lengths, qkv, cos_t, sin_t, k_cache, v_cache, steps):
    batch, slots, heads, head = k_cache.shape
    cols, rows, block = heads * head, steps * batch, 4
    k_t, v_t = jnp.transpose(k_cache, (0, 2, 3, 1)), jnp.transpose(v_cache, (0, 2, 3, 1))
    src = jnp.arange(cols)[:, None]
    dst = jnp.arange(cols)[None, :]
    low = dst % head < head // 2
    swap = (jnp.where(low & (src == dst + head // 2), -1.0, 0.0) + jnp.where(~low & (src == dst - head // 2), 1.0, 0.0)).astype(BF16)
    whole = lambda shape: pl.BlockSpec(shape, lambda i: (0,) * len(shape))
    cache_blk = pl.BlockSpec((block, heads, head, slots), lambda i: (i, 0, 0, 0))
    o, k_o, v_o = pl.pallas_call(
        functools.partial(attention_kernel, steps, batch, block, heads, head),
        grid=(batch // block,),
        in_specs=[pl.BlockSpec(memory_space=pltpu.SMEM), whole((rows, 3 * cols)), whole((rows, cols)), whole((rows, cols)), whole((cols, cols)), cache_blk, cache_blk],
        out_specs=[whole((rows, cols)), cache_blk, cache_blk],
        out_shape=[jax.ShapeDtypeStruct((rows, cols), BF16), jax.ShapeDtypeStruct(k_t.shape, BF16), jax.ShapeDtypeStruct(v_t.shape, BF16)],
        scratch_shapes=[pltpu.VMEM((steps, batch, cols), F32), pltpu.VMEM((cols, rows), BF16), pltpu.VMEM((cols, rows), BF16), pltpu.VMEM((steps, batch, cols), F32)],
        compiler_params=pltpu.CompilerParams(dimension_semantics=("arbitrary",)),
        cost_estimate=pl.CostEstimate(flops=4 * 10 ** 9, bytes_accessed=4 * k_t.size * 2, transcendentals=0),
        name="attention",
    )(lengths, qkv, cos_t, sin_t, swap, k_t, v_t)
    back = lambda a: jnp.transpose(a, (0, 3, 1, 2))
    return o, back(k_o), back(v_o)


def rope_tables(lengths, steps, heads, head):
    half = head // 2
    inv_freq = ROPE_BASE ** (-(jnp.arange(half, dtype=F32) * 2.0 / head))
    positions = (lengths[None, :] + jnp.arange(steps)[:, None]).reshape(-1).astype(F32)
    angles = positions[:, None] * inv_freq[None, :]
    tile = lambda a: jnp.concatenate([a] * (2 * heads), axis=1)
    return tile(jnp.cos(angles)), tile(jnp.sin(angles))


def shard_norm(x_val, gain_vec, width_full):
    x_f32 = x_val.astype(F32)
    sq_total = lax.psum(jnp.sum(x_f32 * x_f32, axis=-1, keepdims=True), 'x')
    return (x_f32 * lax.rsqrt(sq_total / width_full + EPS) * gain_vec.astype(F32)).astype(BF16)


def solution(mesh):
    x_count = mesh.shape['x']
    cache_spec = P('dp', None, 'y', None)
    in_specs = (P(None, 'dp'), P('dp'), P(None, 'dp', None), P(None, 'x'), cache_spec, cache_spec, P('x'), P('x', 'y'), P('x', 'y'), P('x', 'y'), P('y', 'x'), P('x'), P('x', None), P(None, 'x', 'y'), P(None, 'x', 'y'), P(None, 'y', 'x'))
    out_specs = (P(None, 'dp', 'x'), cache_spec, cache_spec)

    def per_device(tokens, lengths, choices, emb_table, k_cache, v_cache, g_attn, w_q, w_k, w_v, w_o, g_ffn, w_router, w_act, w_lin, w_down):
        steps, n_batch = tokens.shape
        heads, head = k_cache.shape[2], k_cache.shape[3]
        rows = steps * n_batch
        width_full = emb_table.shape[1] * x_count
        experts, width, ff = w_act.shape
        cos_t, sin_t = rope_tables(lengths, steps, heads, head)
        x_in = jnp.take(emb_table, tokens.reshape(rows), axis=0)
        normed = shard_norm(x_in, g_attn, width_full)
        qkv_part = jnp.concatenate([dot(normed, w_q), dot(normed, w_k), dot(normed, w_v)], axis=1).astype(BF16)
        qkv = lax.psum(qkv_part, 'x')
        mixed, k_out, v_out = attention(lengths, qkv, cos_t, sin_t, k_cache, v_cache, steps)
        attn_sum = lax.psum(dot(mixed, w_o).astype(BF16), 'y')
        x_mid = (x_in.astype(F32) + attn_sum.astype(F32)).astype(BF16)
        normed2 = shard_norm(x_mid, g_ffn, width_full)
        logits = lax.psum(dot(normed2, w_router), 'x')
        choice = choices.reshape(rows, 2)
        hot = choice[:, :, None] == jnp.arange(experts)[None, None, :]
        picked = jnp.sum(jnp.where(hot, logits[:, None, :], 0.0), axis=-1)
        gate = jax.nn.softmax(picked, axis=-1)
        hot_t = jnp.transpose(hot, (1, 0, 2))
        sparse = jnp.where(hot_t[..., None], normed2[None, :, None, :], 0).reshape(2 * rows, experts * width)
        hid_part = jnp.stack([dot(sparse, w_act.reshape(experts * width, ff)), dot(sparse, w_lin.reshape(experts * width, ff))]).astype(BF16)
        hid = lax.psum(hid_part, 'x').astype(F32)
        unit = (gate.T.reshape(2 * rows, 1) * jax.nn.silu(hid[0]) * hid[1]).astype(BF16).reshape(2, rows, ff)
        unit_e = jnp.sum(jnp.where(jnp.transpose(hot_t, (2, 0, 1))[..., None], unit[None], 0), axis=1)
        moe = lax.psum(jnp.einsum('ebf,efd->bd', unit_e, w_down, preferred_element_type=F32).astype(BF16), 'y')
        out = (x_mid.astype(F32) + moe.astype(F32)).astype(BF16)
        return out.reshape(steps, n_batch, width), k_out, v_out

    return jax.shard_map(per_device, mesh=mesh, in_specs=in_specs, out_specs=out_specs, check_vma=False)
```

```python
import functools
import jax
import jax.numpy as jnp
from jax import lax
from jax.experimental import pallas as pl
from jax.experimental.pallas import tpu as pltpu
from jax.sharding import PartitionSpec as P

EPS = 1e-5
ROPE_BASE = 1.0e6
F32 = jnp.float32
BF16 = jnp.bfloat16
LANES = 128


def dot(a, b):
    return lax.dot_general(a, b, (((1,), (0,)), ((), ())), preferred_element_type=F32)


def dot_nt(a, b):
    return lax.dot_general(a, b, (((1,), (1,)), ((), ())), preferred_element_type=F32)


def gather_kernel(rows, vocab, depth, tok_ref, tok_col, last_ref, emb_ref, x_ref, buf, acc, sem):
    tiles = vocab // LANES

    def copy(i):
        tile = jnp.minimum(tok_ref[i] // LANES, tiles - 1)
        src = emb_ref.at[:, pl.ds(pl.multiple_of(tile * LANES, LANES), LANES)]
        slot = lax.rem(i, depth)
        return pltpu.make_async_copy(src, buf.at[slot], sem.at[slot])

    @pl.loop(0, depth)
    def _(i):
        copy(i).start()

    lane_id = lax.broadcasted_iota(jnp.int32, acc.shape[1:], 1)

    @pl.loop(0, rows)
    def _(i):
        copy(i).wait()
        lane, group = lax.rem(i, LANES), i // LANES
        shift = lax.rem(lane - lax.rem(tok_ref[i], LANES) + LANES, LANES)
        moved = pltpu.roll(buf[lax.rem(i, depth)].astype(acc.dtype), shift, 1)
        acc[group] = jnp.where(lane_id == lane, moved, acc[group])

        @pl.when(i + depth < rows)
        def _():
            copy(i + depth).start()

    groups = pl.cdiv(rows, LANES)
    x_all = jnp.concatenate([acc[g].astype(F32).T for g in range(groups)], axis=0)[:rows]
    x_ref[...] = jnp.where(tok_col[...] >= tiles * LANES, last_ref[...].astype(F32), x_all).astype(BF16)


def gather(emb_table, tokens, acc_dtype=BF16, depth=32):
    vocab, width = emb_table.shape
    rows = tokens.shape[0]
    vmem = pl.BlockSpec(memory_space=pltpu.VMEM)
    tiles = vocab // LANES
    last = lax.slice(emb_table, (vocab - 1, 0), (vocab, width))
    assert vocab - tiles * LANES == 1
    return pl.pallas_call(
        functools.partial(gather_kernel, rows, vocab, depth),
        in_specs=[pl.BlockSpec(memory_space=pltpu.SMEM), vmem, vmem, pl.BlockSpec(memory_space=pl.ANY)],
        out_specs=vmem,
        out_shape=jax.ShapeDtypeStruct((rows, width), BF16),
        scratch_shapes=[pltpu.VMEM((depth, width, LANES), BF16), pltpu.VMEM((pl.cdiv(rows, LANES), width, LANES), acc_dtype), pltpu.SemaphoreType.DMA((depth,))],
        name="gather",
    )(tokens, tokens[:, None], last, emb_table.T)


def attention_kernel(steps, batch, block, heads, head, lens_ref, kvq_ref, cos_ref, sin_ref, swap_ref, k_in, v_in, o_ref, k_out, v_out, q_rows, kt_ref, vt_ref, o_rows):
    cols = heads * head
    slots = k_in.shape[-1]
    rows = steps * batch
    i = pl.program_id(0)
    hpad = 16
    per_group = slots // 4

    @pl.when(i == 0)
    def _():
        cosine, sine = cos_ref[...], sin_ref[...]
        row = lax.broadcasted_iota(jnp.int32, (rows, 4 * batch), 0)
        col = lax.broadcasted_iota(jnp.int32, (rows, 4 * batch), 1)
        perm = jnp.where((row // batch == col % 4) & (row % batch == col // 4), 1.0, 0.0).astype(BF16)
        for part in (2, 0):
            val = kvq_ref[part]
            swapped = dot(val, swap_ref[...])
            rot = (val.astype(F32) * cosine + swapped * sine).astype(BF16).astype(F32)
            if part == 2:
                q_rows[...] = rot.reshape(steps, batch, cols)
            else:
                kt = dot(rot.T.astype(BF16), perm)
        vt = dot(kvq_ref[1].astype(F32).T.astype(BF16), perm)
        for g in range(batch // per_group):
            kt_ref[g] = kt[:, g * slots:(g + 1) * slots].astype(kt_ref.dtype)
            vt_ref[g] = vt[:, g * slots:(g + 1) * slots].astype(vt_ref.dtype)

    head_mask = lax.broadcasted_iota(jnp.int32, (hpad, cols), 1) // head == lax.broadcasted_iota(jnp.int32, (hpad, cols), 0)
    t_of = lax.broadcasted_iota(jnp.int32, (steps * hpad, slots), 0) // hpad
    s_of = lax.broadcasted_iota(jnp.int32, (steps * hpad, slots), 1)
    slot_id = lax.broadcasted_iota(jnp.int32, (cols, slots), 1)

    group = (i * block) // per_group
    news, scores_all = [], []
    for n in range(block):
        b = i * block + n
        first = lens_ref[b]
        shift = lax.rem(first - 4 * lax.rem(b, per_group) + slots, slots)
        fresh = (slot_id >= first) & (slot_id < first + steps)
        k_new = jnp.where(fresh, pltpu.roll(kt_ref[group], shift, 1).astype(BF16), k_in[n].reshape(cols, slots))
        v_new = jnp.where(fresh, pltpu.roll(vt_ref[group], shift, 1).astype(BF16), v_in[n].reshape(cols, slots))
        k_out[n] = k_new.reshape(heads, head, slots)
        v_out[n] = v_new.reshape(heads, head, slots)
        q_blk = jnp.concatenate([jnp.where(head_mask, jnp.broadcast_to(q_rows[t, pl.ds(b, 1), :], (hpad, cols)), 0.0) for t in range(steps)], axis=0).astype(BF16)
        scores = dot(q_blk, k_new) * head ** -0.5
        scores_all.append(jnp.where(s_of <= first + t_of, scores, -1.0e30))
        news.append(v_new)
    scores = jnp.concatenate(scores_all, axis=0)
    peak = jnp.max(scores, axis=-1, keepdims=True)
    weight = jnp.exp(scores - peak)
    total = jnp.sum(weight, axis=-1, keepdims=True)
    weight = weight.astype(BF16)
    span = steps * hpad
    for n in range(block):
        b = i * block + n
        mixed = dot_nt(weight[n * span:(n + 1) * span], news[n]) / total[n * span:(n + 1) * span]
        for t in range(steps):
            o_rows[t, pl.ds(b, 1), :] = jnp.sum(jnp.where(head_mask, mixed[t * hpad:(t + 1) * hpad], 0.0), axis=0, keepdims=True)

    @pl.when(i == pl.num_programs(0) - 1)
    def _():
        o_ref[...] = o_rows[...].reshape(rows, cols).astype(BF16)


def attention(lengths, kvq, cos_t, sin_t, k_cache, v_cache, steps, block=16, roll_dtype=BF16):
    batch, slots, heads, head = k_cache.shape
    cols, rows = heads * head, steps * batch
    k_t, v_t = jnp.transpose(k_cache, (0, 2, 3, 1)), jnp.transpose(v_cache, (0, 2, 3, 1))
    src = jnp.arange(cols)[:, None]
    dst = jnp.arange(cols)[None, :]
    low = dst % head < head // 2
    swap = (jnp.where(low & (src == dst + head // 2), -1.0, 0.0) + jnp.where(~low & (src == dst - head // 2), 1.0, 0.0)).astype(BF16)
    whole = lambda shape: pl.BlockSpec(shape, lambda i: (0,) * len(shape))
    cache_blk = pl.BlockSpec((block, heads, head, slots), lambda i: (i, 0, 0, 0))
    groups = 4 * batch // slots
    o, k_o, v_o = pl.pallas_call(
        functools.partial(attention_kernel, steps, batch, block, heads, head),
        grid=(batch // block,),
        in_specs=[pl.BlockSpec(memory_space=pltpu.SMEM), whole((3, rows, cols)), whole((rows, cols)), whole((rows, cols)), whole((cols, cols)), cache_blk, cache_blk],
        out_specs=[whole((rows, cols)), cache_blk, cache_blk],
        out_shape=[jax.ShapeDtypeStruct((rows, cols), BF16), jax.ShapeDtypeStruct(k_t.shape, BF16), jax.ShapeDtypeStruct(v_t.shape, BF16)],
        scratch_shapes=[pltpu.VMEM((steps, batch, cols), F32), pltpu.VMEM((groups, cols, slots), roll_dtype), pltpu.VMEM((groups, cols, slots), roll_dtype), pltpu.VMEM((steps, batch, cols), F32)],
        compiler_params=pltpu.CompilerParams(dimension_semantics=("arbitrary",)),
        cost_estimate=pl.CostEstimate(flops=4 * 10 ** 9, bytes_accessed=4 * k_t.size * 2, transcendentals=0),
        name="attention",
    )(lengths, kvq, cos_t, sin_t, swap, k_t, v_t)
    back = lambda a: jnp.transpose(a, (0, 3, 1, 2))
    return o, back(k_o), back(v_o)


X, Y = 'x', 'y'
MESH = pl.DeviceIdType.MESH


def positions():
    xi, yi = lax.axis_index(X), lax.axis_index(Y)
    core, chip = lax.rem(xi, 2), xi // 2
    pair = xi + 1 - 2 * core
    cross = lax.rem(xi + 2, 4)
    diag = lax.rem(pair + 2, 4)
    return xi, yi, core, chip, pair, cross, diag


def enter(x_peers, yi, y_count):
    barrier = pltpu.get_barrier_semaphore()
    for peer in x_peers:
        pl.semaphore_signal(barrier, inc=1, device_id={X: peer}, device_id_type=MESH)
    for d in range(1, y_count):
        pl.semaphore_signal(barrier, inc=1, device_id={Y: lax.rem(yi + d, y_count)}, device_id_type=MESH)
    pl.semaphore_wait(barrier, len(x_peers) + y_count - 1)


def remote(src, dst, send, recv, **where):
    return pltpu.make_async_remote_copy(src_ref=src, dst_ref=dst, send_sem=send, recv_sem=recv, device_id=where, device_id_type=MESH)


def start_all(copies):
    for c in copies:
        c.start()
    return copies


def scatter_y(src, dst, sems, yi, y_count, span):
    out = []
    for d in range(1, y_count):
        peer = lax.rem(yi + d, y_count)
        rows = pl.ds(pl.multiple_of(peer * span, span), span)
        out.append(remote(src.at[rows], dst.at[d - 1], sems.at[0, d - 1], sems.at[1, d - 1], y=peer))
    return start_all(out)


def gather_y(src, dst, sems, yi, y_count, span):
    rows = pl.ds(pl.multiple_of(yi * span, span), span)
    return start_all([remote(src, dst.at[rows], sems.at[0, d - 1], sems.at[1, d - 1], y=lax.rem(yi + d, y_count)) for d in range(1, y_count)])


def normalise(x_f32, gain, stat, stat_in, sems, peers, width_full):
    rows = x_f32.shape[0]
    part = jnp.sum(x_f32 * x_f32, axis=-1, keepdims=True)
    stat[:, :rows] = jnp.broadcast_to(part, (rows, LANES)).T[:8]
    copies = start_all([remote(stat, stat_in.at[i], sems.at[0, i], sems.at[1, i], x=peer) for i, peer in enumerate(peers)])
    for c in copies:
        c.wait()
    total = ((stat[...] + stat_in[0]) + (stat_in[1] + stat_in[2])).T[:rows, :1]
    return (x_f32 * lax.rsqrt(total / width_full + EPS) * gain).astype(BF16)


def qkv_kernel(y_count, width_full, x_ref, g_ref, wk_ref, wv_ref, wq_ref, out_ref, stat, stat_in, h_own, h_all, keep, snd1, rcv1, snd2, rcv2, done, rcv3, stat_sem, y_sem, s1, s2, s3):
    xi, yi, core, chip, pair, cross, diag = positions()
    span, rows = x_ref.shape[0], h_all.shape[0]
    half = rows // 2
    stat[...] = jnp.zeros_like(stat)
    enter((pair, cross, diag), yi, y_count)
    h = normalise(x_ref[...].astype(F32), g_ref[...].astype(F32), stat, stat_in, stat_sem, (pair, cross, diag), width_full)
    h_own[...] = h
    sent = gather_y(h_own, h_all, y_sem, yi, y_count, span)
    h_all[pl.ds(pl.multiple_of(yi * span, span), span)] = h
    for c in sent:
        c.wait()
    mine = pl.ds(pl.multiple_of(core * half, half), half)
    theirs = pl.ds(pl.multiple_of((1 - core) * half, half), half)
    first, second, third = [], [], []
    weights = (wk_ref, wv_ref, wq_ref)
    for m in range(3):
        snd1[m] = dot(h_all[theirs], weights[m][...]).astype(BF16)
        first += start_all([remote(snd1.at[m], rcv1.at[m], s1.at[0, m], s1.at[1, m], x=pair)])
        keep[m] = dot(h_all[mine], weights[m][...])
        first[m].wait_recv()
        snd2[m] = (keep[m] + rcv1[m].astype(F32)).astype(BF16)
        second += start_all([remote(snd2.at[m], rcv2.at[m], s2.at[0, m], s2.at[1, m], x=cross)])
    for m in range(3):
        second[m].wait_recv()
        done[m] = (snd2[m].astype(F32) + rcv2[m].astype(F32)).astype(BF16)
        third += start_all([remote(done.at[m], rcv3.at[m], s3.at[0, m], s3.at[1, m], x=pair)])
        out_ref[m, mine] = done[m]
    for m in range(3):
        third[m].wait_recv()
        out_ref[m, theirs] = rcv3[m]
    for c in first + second + third:
        c.wait_send()


def qkv_sums(x_own, gain, w_q, w_k, w_v, rows, y_count, width_full):
    span, width = x_own.shape
    cols, half = w_q.shape[1], rows // 2
    vmem = pl.BlockSpec(memory_space=pltpu.VMEM)
    part = pltpu.VMEM((3, half, cols), BF16)
    pairs = pltpu.SemaphoreType.DMA((2, 3))
    return pl.pallas_call(
        functools.partial(qkv_kernel, y_count, width_full),
        in_specs=[vmem] * 5,
        out_specs=vmem,
        out_shape=jax.ShapeDtypeStruct((3, rows, cols), BF16),
        scratch_shapes=[pltpu.VMEM((8, LANES), F32), pltpu.VMEM((3, 8, LANES), F32), pltpu.VMEM((span, width), BF16), pltpu.VMEM((rows, width), BF16), pltpu.VMEM((3, half, cols), F32), part, part, part, part, part, part, pairs, pltpu.SemaphoreType.DMA((2, y_count - 1)), pairs, pairs, pairs],
        compiler_params=pltpu.CompilerParams(collective_id=0, has_side_effects=True),
        cost_estimate=pl.CostEstimate(flops=6 * rows * width * cols, bytes_accessed=8 * width * cols, transcendentals=0),
        name="qkv_sums",
    )(x_own, gain[None, :], w_k, w_v, w_q)


def chunks_of(ff, wide):
    return tuple((lo, min(wide, ff - lo)) for lo in range(0, ff, wide))


def moe_kernel(y_count, width_full, chunks, experts, o_ref, wo_ref, x_ref, g_ref, wr_ref, ch_ref, act_hbm, lin_hbm, down_hbm, out_ref, act, lin, down, stat, stat_in, part, rs_in, h_own, h_all, logit, logit_in, gate, mask, sparse, acc_down, x_mid, *rest):
    n_chunk = len(chunks)
    keep, snd1, rcv1, snd2, rcv2, u_mine, u_pair = [rest[i * n_chunk:(i + 1) * n_chunk] for i in range(7)]
    w_sem, stat_sem, rs_sem, ag_sem, lg_sem, s1, s2, s3, s4, s5, rs2_sem, ag2_sem = rest[7 * n_chunk:]
    xi, yi, core, chip, pair, cross, diag = positions()
    peers = (pair, cross, diag)
    span, rows = x_ref.shape[0], h_all.shape[0]
    half, width = rows // 2, x_ref.shape[1]
    loads = []
    for i, (src, dst) in enumerate(((act_hbm, act), (lin_hbm, lin), (down_hbm, down))):
        for e in range(experts):
            loads.append(pltpu.make_async_copy(src.at[e], dst.at[e], w_sem.at[i, e]))
    start_all(loads)
    stat[...] = jnp.zeros_like(stat)
    logit[...] = jnp.zeros_like(logit)
    enter(peers, yi, y_count)

    own = pl.ds(pl.multiple_of(yi * span, span), span)
    part[...] = dot(o_ref[...], wo_ref[...]).astype(BF16)
    sent = scatter_y(part, rs_in, rs_sem, yi, y_count, span)
    ch = ch_ref[...]
    ch_keep = jnp.where(core == 0, ch[:, :1], ch[:, 1:])
    ch_send = jnp.where(core == 0, ch[:, 1:], ch[:, :1])
    for e in range(experts):
        mask[0, e] = jnp.broadcast_to(jnp.where(ch_keep == e, 1.0, 0.0), (rows, LANES)).astype(BF16)
        mask[1, e] = jnp.broadcast_to(jnp.where(ch_send == e, 1.0, 0.0), (rows, LANES)).astype(BF16)

    def wide_mask(s, e, n):
        return jnp.concatenate([mask[s, e]] * (n // LANES) + ([mask[s, e][:, :n % LANES]] if n % LANES else []), axis=1)

    for c in sent:
        c.wait()
    total = part[own].astype(F32) + rs_in[0].astype(F32) + rs_in[1].astype(F32) + rs_in[2].astype(F32)
    x_new = (x_ref[...].astype(F32) + total).astype(BF16)
    x_mid[...] = x_new
    h = normalise(x_new.astype(F32), g_ref[...].astype(F32), stat, stat_in, stat_sem, peers, width_full)
    h_own[...] = h
    sent = gather_y(h_own, h_all, ag_sem, yi, y_count, span)
    h_all[own] = h
    for c in sent:
        c.wait()
    logit[:, :rows] = dot_nt(wr_ref[...], h_all[...])
    lg = start_all([remote(logit, logit_in.at[i], lg_sem.at[0, i], lg_sem.at[1, i], x=peer) for i, peer in enumerate(peers)])
    h2 = h_all[...]
    for e in range(experts):
        for s in range(2):
            sparse[s, e] = h2 * wide_mask(s, e, width)

    for copy in loads[:2 * experts]:
        copy.wait()

    mine = pl.ds(pl.multiple_of(chip * half, half), half)
    other = pl.ds(pl.multiple_of((1 - chip) * half, half), half)
    first, second, to_cross, to_pair, forward = [], [], [], [], []

    def product(s, w, lo, n):
        def body(e, acc):
            return acc + dot(sparse[s, e], w[e, :, lo:lo + n])
        return lax.fori_loop(0, experts, body, jnp.zeros((rows, n), F32))

    def sums(k):
        lo, n = chunks[k]
        snd1[k][0] = product(1, act, lo, n).astype(BF16)
        snd1[k][1] = product(1, lin, lo, n).astype(BF16)
        first.extend(start_all([remote(snd1[k], rcv1[k], s1.at[0, k], s1.at[1, k], x=pair)]))
        keep[k][0] = product(0, act, lo, n)
        keep[k][1] = product(0, lin, lo, n)
        first[k].wait_recv()
        for i in range(2):
            snd2[k][i] = (keep[k][i, other] + rcv1[k][i, other].astype(F32)).astype(BF16)
        second.extend(start_all([remote(snd2[k], rcv2[k], s2.at[0, k], s2.at[1, k], x=cross)]))
        for i in range(2):
            keep[k][i, mine] = keep[k][i, mine] + rcv1[k][i, mine].astype(F32)

    def gates():
        for c in lg:
            c.wait()
        logits = ((logit[...] + logit_in[0]) + (logit_in[1] + logit_in[2])).T[:rows]
        col = lax.broadcasted_iota(jnp.int32, logits.shape, 1)
        l_keep = jnp.sum(jnp.where(col == ch_keep, logits, 0.0), axis=1, keepdims=True)
        l_send = jnp.sum(jnp.where(col == ch_send, logits, 0.0), axis=1, keepdims=True)
        top = jnp.maximum(l_keep, l_send)
        e_keep, e_send = jnp.exp(l_keep - top), jnp.exp(l_send - top)
        gate[...] = jnp.broadcast_to(e_keep / (e_keep + e_send), gate.shape)

    def unit(k):
        second[k].wait_recv()
        a = keep[k][0, mine] + rcv2[k][0].astype(F32)
        b = keep[k][1, mine] + rcv2[k][1].astype(F32)
        u_mine[k][mine] = (gate[mine][:, :1] * (a * jax.nn.sigmoid(a)) * b).astype(BF16)
        to_cross.extend(start_all([remote(u_mine[k].at[mine], u_mine[k].at[mine], s3.at[0, k], s3.at[1, k], x=cross)]))
        to_pair.extend(start_all([remote(u_mine[k].at[mine], u_pair[k].at[mine], s4.at[0, k], s4.at[1, k], x=pair)]))

    def pass_on(k):
        to_cross[k].wait_recv()
        forward.extend(start_all([remote(u_mine[k].at[other], u_pair[k].at[other], s5.at[0, k], s5.at[1, k], x=pair)]))

    def downward(k):
        lo, n = chunks[k]
        to_pair[k].wait_recv()
        forward[k].wait_recv()
        u0, u1 = u_mine[k][...], u_pair[k][...]
        total = jnp.zeros((rows, width), F32) if k == 0 else acc_down[...]
        for e in range(experts):
            total = total + dot_nt(u0 * wide_mask(0, e, n) + u1 * wide_mask(1, e, n), down[e, :, lo:lo + n])
        acc_down[...] = total

    sums(0)
    sums(1)
    gates()
    sums(2)
    unit(0)
    for k in range(3, n_chunk):
        sums(k)
    unit(1)
    pass_on(0)
    for copy in loads[2 * experts:]:
        copy.wait()
    for k in range(2, n_chunk):
        unit(k)
        pass_on(k - 1)
        downward(k - 2)
    pass_on(n_chunk - 1)
    downward(n_chunk - 2)
    downward(n_chunk - 1)

    part[...] = acc_down[...].astype(BF16)
    sent = scatter_y(part, rs_in, rs2_sem, yi, y_count, span)
    for c in sent:
        c.wait()
    total = part[own].astype(F32) + rs_in[0].astype(F32) + rs_in[1].astype(F32) + rs_in[2].astype(F32)
    h_new = (x_mid[...].astype(F32) + total).astype(BF16)
    h_own[...] = h_new
    sent = gather_y(h_own, h_all, ag2_sem, yi, y_count, span)
    h_all[own] = h_new
    for c in sent:
        c.wait()
    out_ref[...] = h_all[...]
    for c in first + second + to_cross + to_pair + forward:
        c.wait_send()


def moe(mixed, w_o, x_own, gain, w_router, choice, w_act, w_lin, w_down, y_count, width_full):
    rows, heads = mixed.shape
    span, width = x_own.shape
    experts, _, ff = w_act.shape
    half, chunks = rows // 2, chunks_of(ff, 384)
    vmem, hbm = pl.BlockSpec(memory_space=pltpu.VMEM), pl.BlockSpec(memory_space=pl.ANY)
    down_t = jnp.transpose(w_down, (0, 2, 1))
    three = pltpu.SemaphoreType.DMA((2, 3))
    ring = pltpu.SemaphoreType.DMA((2, y_count - 1))
    per_chunk = pltpu.SemaphoreType.DMA((2, len(chunks)))
    buf = lambda lead, r, dt: [pltpu.VMEM(lead + (r, n), dt) for _, n in chunks]
    scratch = [pltpu.VMEM(w_act.shape, BF16), pltpu.VMEM(w_act.shape, BF16), pltpu.VMEM(down_t.shape, BF16), pltpu.VMEM((8, LANES), F32), pltpu.VMEM((3, 8, LANES), F32), pltpu.VMEM((rows, width), BF16), pltpu.VMEM((y_count - 1, span, width), BF16), pltpu.VMEM((span, width), BF16), pltpu.VMEM((rows, width), BF16), pltpu.VMEM((experts, 2 * LANES), F32), pltpu.VMEM((3, experts, 2 * LANES), F32), pltpu.VMEM((rows, LANES), F32), pltpu.VMEM((2, experts, rows, LANES), BF16), pltpu.VMEM((2, experts, rows, width), BF16), pltpu.VMEM((rows, width), F32), pltpu.VMEM((span, width), BF16)]
    scratch += buf((2,), rows, F32) + buf((2,), rows, BF16) + buf((2,), rows, BF16) + buf((2,), half, BF16) + buf((2,), half, BF16) + buf((), rows, BF16) + buf((), rows, BF16)
    scratch += [pltpu.SemaphoreType.DMA((3, experts)), three, ring, ring, three] + [per_chunk] * 5 + [ring, ring]
    return pl.pallas_call(
        functools.partial(moe_kernel, y_count, width_full, chunks, experts),
        in_specs=[vmem] * 6 + [hbm] * 3,
        out_specs=vmem,
        out_shape=jax.ShapeDtypeStruct((rows, width), BF16),
        scratch_shapes=scratch,
        compiler_params=pltpu.CompilerParams(collective_id=1, has_side_effects=True, vmem_limit_bytes=67043328),
        cost_estimate=pl.CostEstimate(flops=2 * 10 ** 10, bytes_accessed=6 * w_act.size, transcendentals=0),
        name="moe",
    )(mixed, w_o, x_own, gain[None, :], w_router.T, choice, w_act, w_lin, down_t)


def rope_tables(lengths, steps, heads, head):
    half = head // 2
    inv_freq = ROPE_BASE ** (-(jnp.arange(half, dtype=F32) * 2.0 / head))
    spots = (lengths[None, :] + jnp.arange(steps)[:, None]).reshape(-1).astype(F32)
    angles = spots[:, None] * inv_freq[None, :]
    tile = lambda a: jnp.concatenate([a] * (2 * heads), axis=1)
    return tile(jnp.cos(angles)), tile(jnp.sin(angles))


def solution(mesh):
    x_count, y_count = mesh.shape['x'], mesh.shape['y']
    assert x_count == 4 and y_count == 4
    cache_spec = P('dp', None, 'y', None)
    in_specs = (P(None, 'dp'), P('dp'), P(None, 'dp', None), P(None, 'x'), cache_spec, cache_spec, P('x'), P('x', 'y'), P('x', 'y'), P('x', 'y'), P('y', 'x'), P('x'), P('x', None), P(None, 'x', 'y'), P(None, 'x', 'y'), P(None, 'y', 'x'))
    out_specs = (P(None, 'dp', 'x'), cache_spec, cache_spec)

    def per_device(tokens, lengths, choices, emb_table, k_cache, v_cache, g_attn, w_q, w_k, w_v, w_o, g_ffn, w_router, w_act, w_lin, w_down):
        steps, n_batch = tokens.shape
        heads, head = k_cache.shape[2], k_cache.shape[3]
        rows = steps * n_batch
        width_full = emb_table.shape[1] * x_count
        span = rows // y_count
        cos_t, sin_t = rope_tables(lengths, steps, heads, head)
        own_tokens = lax.dynamic_slice(tokens.reshape(rows), (lax.axis_index('y') * span,), (span,))
        x_own = gather(emb_table, own_tokens)
        kvq = qkv_sums(x_own, g_attn, w_q, w_k, w_v, rows, y_count, width_full)
        mixed, k_out, v_out = attention(lengths, kvq, cos_t, sin_t, k_cache, v_cache, steps)
        out = moe(mixed, w_o, x_own, g_ffn, w_router, choices.reshape(rows, 2), w_act, w_lin, w_down, y_count, width_full)
        return out.reshape(steps, n_batch, emb_table.shape[1]), k_out, v_out

    return jax.shard_map(per_device, mesh=mesh, in_specs=in_specs, out_specs=out_specs, check_vma=False)
```

```python
import functools
import jax
import jax.numpy as jnp
from jax import lax
from jax.experimental import pallas as pl
from jax.experimental.pallas import tpu as pltpu
from jax.sharding import PartitionSpec as P

EPS = 1e-5
ROPE_BASE = 1.0e6
F32 = jnp.float32
BF16 = jnp.bfloat16
LANES = 128


def dot(a, b):
    return lax.dot_general(a, b, (((1,), (0,)), ((), ())), preferred_element_type=F32)


def dot_nt(a, b):
    return lax.dot_general(a, b, (((1,), (1,)), ((), ())), preferred_element_type=F32)


def gather_kernel(span, vocab, depth, tok_ref, edge_ref, emb_ref, x_ref, buf, acc, sem):
    tiles = vocab // LANES
    batch = tok_ref.shape[1]
    start = lax.axis_index('y') * span

    def token(i):
        r = start + i
        return tok_ref[r // batch, lax.rem(r, batch)]

    def copy(i):
        tile = jnp.minimum(token(i) // LANES, tiles - 1)
        src = emb_ref.at[:, pl.ds(pl.multiple_of(tile * LANES, LANES), LANES)]
        slot = lax.rem(i, depth)
        return pltpu.make_async_copy(src, buf.at[slot], sem.at[slot])

    @pl.loop(0, min(depth, span))
    def _(i):
        copy(i).start()

    lane_id = lax.broadcasted_iota(jnp.int32, acc.shape, 1)

    @pl.loop(0, span)
    def _(i):
        copy(i).wait()
        tok = token(i)
        shift = lax.rem(i - lax.rem(tok, LANES) + LANES, LANES)
        edge = jnp.full(acc.shape, tok, jnp.int32) >= tiles * LANES
        moved = pltpu.roll(jnp.where(edge, edge_ref[...], buf[lax.rem(i, depth)]), shift, 1)
        acc[...] = jnp.where(lane_id == i, moved, acc[...])

        @pl.when(i + depth < span)
        def _():
            copy(i + depth).start()

    x_ref[...] = acc[...].astype(F32).T[:span].astype(BF16)


def gather(emb_table, tokens, span, depth=48):
    vocab, width = emb_table.shape
    table = emb_table.T
    return pl.pallas_call(
        functools.partial(gather_kernel, span, vocab, depth),
        grid=(1,),
        in_specs=[pl.BlockSpec(memory_space=pltpu.SMEM), pl.BlockSpec((width, LANES), lambda i: (0, vocab // LANES)), pl.BlockSpec(memory_space=pl.ANY)],
        out_specs=pl.BlockSpec((span, width), lambda i: (0, 0)),
        out_shape=jax.ShapeDtypeStruct((span, width), BF16),
        scratch_shapes=[pltpu.VMEM((depth, width, LANES), BF16), pltpu.VMEM((width, LANES), BF16), pltpu.SemaphoreType.DMA((depth,))],
        name="gather",
    )(tokens, table, table)


def attention_kernel(steps, batch, block, heads, head, lens_ref, kvq_ref, cos_ref, sin_ref, k_in, v_in, o_ref, k_out, v_out, q_rows, kt_ref, vt_ref, o_rows):
    cols = heads * head
    slots = k_in.shape[-1]
    rows = steps * batch
    i = pl.program_id(0)
    hpad = 16
    per_group = slots // 4

    @pl.when(i == 0)
    def _():
        def spread(table):
            four = jnp.concatenate([table] * (LANES // table.shape[1]), axis=1)
            return jnp.concatenate([four] * (cols // LANES) + [four[:, :cols % LANES]], axis=1)

        cosine, sine = spread(cos_ref[...]), spread(sin_ref[...])
        src = lax.broadcasted_iota(jnp.int32, (cols, cols), 0)
        dst = lax.broadcasted_iota(jnp.int32, (cols, cols), 1)
        low = dst % head < head // 2
        swap = jnp.where(low & (src == dst + head // 2), -1.0, jnp.where(~low & (src == dst - head // 2), 1.0, 0.0)).astype(BF16)
        row = lax.broadcasted_iota(jnp.int32, (rows, 4 * batch), 0)
        col = lax.broadcasted_iota(jnp.int32, (rows, 4 * batch), 1)
        perm = jnp.where((row // batch == col % 4) & (row % batch == col // 4), 1.0, 0.0).astype(BF16)
        for part in (2, 0):
            val = kvq_ref[part]
            swapped = dot(val, swap)
            rot = (val.astype(F32) * cosine + swapped * sine).astype(BF16).astype(F32)
            if part == 2:
                q_rows[...] = rot.reshape(steps, batch, cols)
            else:
                kt = dot(rot.T.astype(BF16), perm)
        vt = dot(kvq_ref[1].astype(F32).T.astype(BF16), perm)
        for g in range(batch // per_group):
            kt_ref[g] = kt[:, g * slots:(g + 1) * slots].astype(kt_ref.dtype)
            vt_ref[g] = vt[:, g * slots:(g + 1) * slots].astype(vt_ref.dtype)

    head_mask = lax.broadcasted_iota(jnp.int32, (hpad, cols), 1) // head == lax.broadcasted_iota(jnp.int32, (hpad, cols), 0)
    t_of = lax.broadcasted_iota(jnp.int32, (steps * hpad, slots), 0) // hpad
    s_of = lax.broadcasted_iota(jnp.int32, (steps * hpad, slots), 1)
    slot_id = lax.broadcasted_iota(jnp.int32, (cols, slots), 1)

    group = (i * block) // per_group
    news, scores_all = [], []
    for n in range(block):
        b = i * block + n
        first = lens_ref[b]
        shift = lax.rem(first - 4 * lax.rem(b, per_group) + slots, slots)
        fresh = (slot_id >= first) & (slot_id < first + steps)
        k_new = jnp.where(fresh, pltpu.roll(kt_ref[group], shift, 1).astype(BF16), k_in[n].reshape(cols, slots))
        v_new = jnp.where(fresh, pltpu.roll(vt_ref[group], shift, 1).astype(BF16), v_in[n].reshape(cols, slots))
        k_out[n] = k_new.reshape(heads, head, slots)
        v_out[n] = v_new.reshape(heads, head, slots)
        q_blk = jnp.concatenate([jnp.where(head_mask, jnp.broadcast_to(q_rows[t, pl.ds(b, 1), :], (hpad, cols)), 0.0) for t in range(steps)], axis=0).astype(BF16)
        scores = dot(q_blk, k_new) * head ** -0.5
        scores_all.append(jnp.where(s_of <= first + t_of, scores, -1.0e30))
        news.append(v_new)
    scores = jnp.concatenate(scores_all, axis=0)
    peak = jnp.max(scores, axis=-1, keepdims=True)
    weight = jnp.exp(scores - peak)
    total = jnp.sum(weight, axis=-1, keepdims=True)
    weight = weight.astype(BF16)
    span = steps * hpad
    for n in range(block):
        b = i * block + n
        mixed = dot_nt(weight[n * span:(n + 1) * span], news[n]) / total[n * span:(n + 1) * span]
        for t in range(steps):
            o_rows[t, pl.ds(b, 1), :] = jnp.sum(jnp.where(head_mask, mixed[t * hpad:(t + 1) * hpad], 0.0), axis=0, keepdims=True)

    @pl.when(i == pl.num_programs(0) - 1)
    def _():
        o_ref[...] = o_rows[...].reshape(rows, cols).astype(BF16)


def attention(lengths, kvq, cos_t, sin_t, k_cache, v_cache, steps, block=16, roll_dtype=BF16):
    batch, slots, heads, head = k_cache.shape
    cols, rows = heads * head, steps * batch
    k_t, v_t = jnp.transpose(k_cache, (0, 2, 3, 1)), jnp.transpose(v_cache, (0, 2, 3, 1))
    whole = lambda shape: pl.BlockSpec(shape, lambda i: (0,) * len(shape))
    cache_blk = pl.BlockSpec((block, heads, head, slots), lambda i: (i, 0, 0, 0))
    groups = 4 * batch // slots
    o, k_o, v_o = pl.pallas_call(
        functools.partial(attention_kernel, steps, batch, block, heads, head),
        grid=(batch // block,),
        in_specs=[pl.BlockSpec(memory_space=pltpu.SMEM), whole((3, rows, cols)), whole((rows, head // 2)), whole((rows, head // 2)), cache_blk, cache_blk],
        out_specs=[whole((rows, cols)), cache_blk, cache_blk],
        out_shape=[jax.ShapeDtypeStruct((rows, cols), BF16), jax.ShapeDtypeStruct(k_t.shape, BF16), jax.ShapeDtypeStruct(v_t.shape, BF16)],
        scratch_shapes=[pltpu.VMEM((steps, batch, cols), F32), pltpu.VMEM((groups, cols, slots), roll_dtype), pltpu.VMEM((groups, cols, slots), roll_dtype), pltpu.VMEM((steps, batch, cols), F32)],
        compiler_params=pltpu.CompilerParams(dimension_semantics=("arbitrary",)),
        cost_estimate=pl.CostEstimate(flops=4 * 10 ** 9, bytes_accessed=4 * k_t.size * 2, transcendentals=0),
        name="attention",
    )(lengths, kvq, cos_t, sin_t, k_t, v_t)
    back = lambda a: jnp.transpose(a, (0, 3, 1, 2))
    return o, back(k_o), back(v_o)


X, Y = 'x', 'y'
MESH = pl.DeviceIdType.MESH


def positions():
    xi, yi = lax.axis_index(X), lax.axis_index(Y)
    core, chip = lax.rem(xi, 2), xi // 2
    pair = xi + 1 - 2 * core
    cross = lax.rem(xi + 2, 4)
    diag = lax.rem(pair + 2, 4)
    return xi, yi, core, chip, pair, cross, diag


def enter(x_peers, yi, y_count):
    barrier = pltpu.get_barrier_semaphore()
    for peer in x_peers:
        pl.semaphore_signal(barrier, inc=1, device_id={X: peer}, device_id_type=MESH)
    for d in range(1, y_count):
        pl.semaphore_signal(barrier, inc=1, device_id={Y: lax.rem(yi + d, y_count)}, device_id_type=MESH)
    pl.semaphore_wait(barrier, len(x_peers) + y_count - 1)


def remote(src, dst, send, recv, **where):
    return pltpu.make_async_remote_copy(src_ref=src, dst_ref=dst, send_sem=send, recv_sem=recv, device_id=where, device_id_type=MESH)


def start_all(copies):
    for c in copies:
        c.start()
    return copies


def scatter_y(src, dst, sems, yi, y_count, span):
    out = []
    for d in range(1, y_count):
        peer = lax.rem(yi + d, y_count)
        rows = pl.ds(pl.multiple_of(peer * span, span), span)
        out.append(remote(src.at[rows], dst.at[d - 1], sems.at[0, d - 1], sems.at[1, d - 1], y=peer))
    return start_all(out)


def gather_y(src, dst, sems, yi, y_count, span):
    rows = pl.ds(pl.multiple_of(yi * span, span), span)
    return start_all([remote(src, dst.at[rows], sems.at[0, d - 1], sems.at[1, d - 1], y=lax.rem(yi + d, y_count)) for d in range(1, y_count)])


def normalise(x_f32, gain, stat, stat_in, sems, peers, width_full):
    rows = x_f32.shape[0]
    part = jnp.sum(x_f32 * x_f32, axis=-1, keepdims=True)
    stat[:, :rows] = jnp.broadcast_to(part, (rows, LANES)).T[:8]
    copies = start_all([remote(stat, stat_in.at[i], sems.at[0, i], sems.at[1, i], x=peer) for i, peer in enumerate(peers)])
    for c in copies:
        c.wait()
    total = ((stat[...] + stat_in[0]) + (stat_in[1] + stat_in[2])).T[:rows, :1]
    return (x_f32 * lax.rsqrt(total / width_full + EPS) * gain).astype(BF16)


def qkv_kernel(y_count, width_full, x_ref, g_ref, wk_ref, wv_ref, wq_ref, out_ref, stat, stat_in, h_own, h_all, keep, snd1, rcv1, snd2, rcv2, done, rcv3, stat_sem, y_sem, s1, s2, s3):
    xi, yi, core, chip, pair, cross, diag = positions()
    span, rows = x_ref.shape[0], h_all.shape[0]
    half = rows // 2
    stat[...] = jnp.zeros_like(stat)
    enter((pair, cross, diag), yi, y_count)
    h = normalise(x_ref[...].astype(F32), g_ref[...].astype(F32)[None, :], stat, stat_in, stat_sem, (pair, cross, diag), width_full)
    h_own[...] = h
    sent = gather_y(h_own, h_all, y_sem, yi, y_count, span)
    h_all[pl.ds(pl.multiple_of(yi * span, span), span)] = h
    for c in sent:
        c.wait()
    mine = pl.ds(pl.multiple_of(core * half, half), half)
    theirs = pl.ds(pl.multiple_of((1 - core) * half, half), half)
    first, second, third = [], [], []
    weights = (wk_ref, wv_ref, wq_ref)
    for m in range(3):
        snd1[m] = dot(h_all[theirs], weights[m][...]).astype(BF16)
        first += start_all([remote(snd1.at[m], rcv1.at[m], s1.at[0, m], s1.at[1, m], x=pair)])
        keep[m] = dot(h_all[mine], weights[m][...])
        first[m].wait_recv()
        snd2[m] = (keep[m] + rcv1[m].astype(F32)).astype(BF16)
        second += start_all([remote(snd2.at[m], rcv2.at[m], s2.at[0, m], s2.at[1, m], x=cross)])
    for m in range(3):
        second[m].wait_recv()
        done[m] = (snd2[m].astype(F32) + rcv2[m].astype(F32)).astype(BF16)
        third += start_all([remote(done.at[m], rcv3.at[m], s3.at[0, m], s3.at[1, m], x=pair)])
        out_ref[m, mine] = done[m]
    for m in range(3):
        third[m].wait_recv()
        out_ref[m, theirs] = rcv3[m]
    for c in first + second + third:
        c.wait_send()


def qkv_sums(x_own, gain, w_q, w_k, w_v, rows, y_count, width_full):
    span, width = x_own.shape
    cols, half = w_q.shape[1], rows // 2
    vmem = pl.BlockSpec(memory_space=pltpu.VMEM)
    part = pltpu.VMEM((3, half, cols), BF16)
    pairs = pltpu.SemaphoreType.DMA((2, 3))
    return pl.pallas_call(
        functools.partial(qkv_kernel, y_count, width_full),
        in_specs=[vmem] * 5,
        out_specs=vmem,
        out_shape=jax.ShapeDtypeStruct((3, rows, cols), BF16),
        scratch_shapes=[pltpu.VMEM((8, LANES), F32), pltpu.VMEM((3, 8, LANES), F32), pltpu.VMEM((span, width), BF16), pltpu.VMEM((rows, width), BF16), pltpu.VMEM((3, half, cols), F32), part, part, part, part, part, part, pairs, pltpu.SemaphoreType.DMA((2, y_count - 1)), pairs, pairs, pairs],
        compiler_params=pltpu.CompilerParams(collective_id=0, has_side_effects=True),
        cost_estimate=pl.CostEstimate(flops=6 * rows * width * cols, bytes_accessed=8 * width * cols, transcendentals=0),
        name="qkv_sums",
    )(x_own, gain, w_k, w_v, w_q)


def chunks_of(ff, wide):
    return tuple((lo, min(wide, ff - lo)) for lo in range(0, ff, wide))


def moe_kernel(y_count, width_full, chunks, experts, o_ref, wo_ref, x_ref, g_ref, wr_ref, ch_ref, act_hbm, lin_hbm, down_hbm, out_ref, act, lin, down, stat, stat_in, part, rs_in, h_own, h_all, logit, logit_in, gate, mask, sparse, acc_down, x_mid, *rest):
    n_chunk = len(chunks)
    keep, snd1, rcv1, snd2, rcv2, u_mine, u_pair = [rest[i * n_chunk:(i + 1) * n_chunk] for i in range(7)]
    w_sem, stat_sem, rs_sem, ag_sem, lg_sem, s1, s2, s3, s4, s5, rs2_sem, ag2_sem = rest[7 * n_chunk:]
    xi, yi, core, chip, pair, cross, diag = positions()
    peers = (pair, cross, diag)
    span, rows = x_ref.shape[0], h_all.shape[0]
    half, width = rows // 2, x_ref.shape[1]
    loads = []
    for i, (src, dst) in enumerate(((act_hbm, act), (lin_hbm, lin), (down_hbm, down))):
        for e in range(experts):
            place = dst.at[e] if i == 2 else dst.at[pl.ds(e * width, width)]
            loads.append(pltpu.make_async_copy(src.at[e], place, w_sem.at[i, e]))
    start_all(loads)
    stat[...] = jnp.zeros_like(stat)
    logit[...] = jnp.zeros_like(logit)
    enter(peers, yi, y_count)

    own = pl.ds(pl.multiple_of(yi * span, span), span)
    part[...] = dot(o_ref[...], wo_ref[...]).astype(BF16)
    sent = scatter_y(part, rs_in, rs_sem, yi, y_count, span)
    ch = ch_ref[...].astype(F32)
    ch = jnp.concatenate([jnp.concatenate([ch[t], jnp.zeros((8 - ch.shape[1], ch.shape[2]), F32)], axis=0).T for t in range(ch.shape[0])], axis=0)
    ch_keep = jnp.where(core == 0, ch[:, :1], ch[:, 1:2])
    ch_send = jnp.where(core == 0, ch[:, 1:2], ch[:, :1])
    for e in range(experts):
        mask[0, e] = jnp.broadcast_to(jnp.where(ch_keep == e, 1.0, 0.0), (rows, LANES)).astype(BF16)
        mask[1, e] = jnp.broadcast_to(jnp.where(ch_send == e, 1.0, 0.0), (rows, LANES)).astype(BF16)

    def wide_mask(s, e, n):
        return jnp.concatenate([mask[s, e]] * (n // LANES) + ([mask[s, e][:, :n % LANES]] if n % LANES else []), axis=1)

    for c in sent:
        c.wait()
    total = part[own].astype(F32) + rs_in[0].astype(F32) + rs_in[1].astype(F32) + rs_in[2].astype(F32)
    x_new = (x_ref[...].astype(F32) + total).astype(BF16)
    x_mid[...] = x_new
    h = normalise(x_new.astype(F32), g_ref[...].astype(F32)[None, :], stat, stat_in, stat_sem, peers, width_full)
    h_own[...] = h
    sent = gather_y(h_own, h_all, ag_sem, yi, y_count, span)
    h_all[own] = h
    for c in sent:
        c.wait()
    logit[:, :rows] = dot_nt(wr_ref[...], h_all[...])
    lg = start_all([remote(logit, logit_in.at[i], lg_sem.at[0, i], lg_sem.at[1, i], x=peer) for i, peer in enumerate(peers)])
    h2 = h_all[...]
    for e in range(experts):
        for s in range(2):
            sparse[s, :, e * width:(e + 1) * width] = h2 * wide_mask(s, e, width)

    for copy in loads[:2 * experts]:
        copy.wait()

    mine = pl.ds(pl.multiple_of(chip * half, half), half)
    other = pl.ds(pl.multiple_of((1 - chip) * half, half), half)
    first, second, to_cross, to_pair, forward = [], [], [], [], []

    def product(s, w, lo, n):
        return dot(sparse[s], w[:, lo:lo + n])

    def sums(k):
        lo, n = chunks[k]
        snd1[k][0] = product(1, act, lo, n).astype(BF16)
        snd1[k][1] = product(1, lin, lo, n).astype(BF16)
        first.extend(start_all([remote(snd1[k], rcv1[k], s1.at[0, k], s1.at[1, k], x=pair)]))
        keep[k][0] = product(0, act, lo, n)
        keep[k][1] = product(0, lin, lo, n)
        first[k].wait_recv()
        for i in range(2):
            snd2[k][i] = (keep[k][i, other] + rcv1[k][i, other].astype(F32)).astype(BF16)
        second.extend(start_all([remote(snd2[k], rcv2[k], s2.at[0, k], s2.at[1, k], x=cross)]))
        for i in range(2):
            keep[k][i, mine] = keep[k][i, mine] + rcv1[k][i, mine].astype(F32)

    def gates():
        for c in lg:
            c.wait()
        logits = ((logit[...] + logit_in[0]) + (logit_in[1] + logit_in[2])).T[:rows]
        col = lax.broadcasted_iota(jnp.int32, logits.shape, 1).astype(F32)
        l_keep = jnp.sum(jnp.where(col == ch_keep, logits, 0.0), axis=1, keepdims=True)
        l_send = jnp.sum(jnp.where(col == ch_send, logits, 0.0), axis=1, keepdims=True)
        top = jnp.maximum(l_keep, l_send)
        e_keep, e_send = jnp.exp(l_keep - top), jnp.exp(l_send - top)
        gate[...] = jnp.broadcast_to(e_keep / (e_keep + e_send), gate.shape)

    def unit(k):
        second[k].wait_recv()
        a = keep[k][0, mine] + rcv2[k][0].astype(F32)
        b = keep[k][1, mine] + rcv2[k][1].astype(F32)
        u_mine[k][mine] = (gate[mine][:, :1] * (a * jax.nn.sigmoid(a)) * b).astype(BF16)
        to_cross.extend(start_all([remote(u_mine[k].at[mine], u_mine[k].at[mine], s3.at[0, k], s3.at[1, k], x=cross)]))
        to_pair.extend(start_all([remote(u_mine[k].at[mine], u_pair[k].at[mine], s4.at[0, k], s4.at[1, k], x=pair)]))

    def pass_on(k):
        to_cross[k].wait_recv()
        forward.extend(start_all([remote(u_mine[k].at[other], u_pair[k].at[other], s5.at[0, k], s5.at[1, k], x=pair)]))

    def downward(k):
        lo, n = chunks[k]
        to_pair[k].wait_recv()
        forward[k].wait_recv()
        u0, u1 = u_mine[k][...], u_pair[k][...]
        total = jnp.zeros((rows, width), F32) if k == 0 else acc_down[...]
        for e in range(experts):
            total = total + dot_nt(u0 * wide_mask(0, e, n) + u1 * wide_mask(1, e, n), down[e, :, lo:lo + n])
        acc_down[...] = total

    sums(0)
    sums(1)
    gates()
    sums(2)
    for k in range(3, n_chunk):
        unit(k - 3)
        sums(k)
        if k > 3:
            pass_on(k - 4)
    for copy in loads[2 * experts:]:
        copy.wait()
    unit(n_chunk - 3)
    downward(0)
    unit(n_chunk - 2)
    downward(1)
    pass_on(n_chunk - 4)
    unit(n_chunk - 1)
    pass_on(n_chunk - 3)
    for k in range(2, n_chunk - 3):
        downward(k)
    pass_on(n_chunk - 2)
    downward(n_chunk - 3)
    pass_on(n_chunk - 1)
    downward(n_chunk - 2)
    downward(n_chunk - 1)

    part[...] = acc_down[...].astype(BF16)
    sent = scatter_y(part, rs_in, rs2_sem, yi, y_count, span)
    for c in sent:
        c.wait()
    total = part[own].astype(F32) + rs_in[0].astype(F32) + rs_in[1].astype(F32) + rs_in[2].astype(F32)
    h_new = (x_mid[...].astype(F32) + total).astype(BF16)
    h_own[...] = h_new
    sent = gather_y(h_own, h_all, ag2_sem, yi, y_count, span)
    h_all[own] = h_new
    for c in sent:
        c.wait()
    out_ref[...] = h_all[...]
    for c in first + second + to_cross + to_pair + forward:
        c.wait_send()


def moe(mixed, w_o, x_own, gain, w_router, choice, w_act, w_lin, w_down, y_count, width_full):
    rows, heads = mixed.shape
    span, width = x_own.shape
    experts, _, ff = w_act.shape
    half, chunks = rows // 2, chunks_of(ff, 256)
    vmem, hbm = pl.BlockSpec(memory_space=pltpu.VMEM), pl.BlockSpec(memory_space=pl.ANY)
    down_t = jnp.transpose(w_down, (0, 2, 1))
    three = pltpu.SemaphoreType.DMA((2, 3))
    ring = pltpu.SemaphoreType.DMA((2, y_count - 1))
    per_chunk = pltpu.SemaphoreType.DMA((2, len(chunks)))
    buf = lambda lead, r, dt: [pltpu.VMEM(lead + (r, n), dt) for _, n in chunks]
    flat = (experts * width, ff)
    scratch = [pltpu.VMEM(flat, BF16), pltpu.VMEM(flat, BF16), pltpu.VMEM(down_t.shape, BF16), pltpu.VMEM((8, LANES), F32), pltpu.VMEM((3, 8, LANES), F32), pltpu.VMEM((rows, width), BF16), pltpu.VMEM((y_count - 1, span, width), BF16), pltpu.VMEM((span, width), BF16), pltpu.VMEM((rows, width), BF16), pltpu.VMEM((experts, 2 * LANES), F32), pltpu.VMEM((3, experts, 2 * LANES), F32), pltpu.VMEM((rows, LANES), F32), pltpu.VMEM((2, experts, rows, LANES), BF16), pltpu.VMEM((2, rows, experts * width), BF16), pltpu.VMEM((rows, width), F32), pltpu.VMEM((span, width), BF16)]
    scratch += buf((2,), rows, F32) + buf((2,), rows, BF16) + buf((2,), rows, BF16) + buf((2,), half, BF16) + buf((2,), half, BF16) + buf((), rows, BF16) + buf((), rows, BF16)
    scratch += [pltpu.SemaphoreType.DMA((3, experts)), three, ring, ring, three] + [per_chunk] * 5 + [ring, ring]
    return pl.pallas_call(
        functools.partial(moe_kernel, y_count, width_full, chunks, experts),
        in_specs=[vmem] * 6 + [hbm] * 3,
        out_specs=vmem,
        out_shape=jax.ShapeDtypeStruct((rows, width), BF16),
        scratch_shapes=scratch,
        compiler_params=pltpu.CompilerParams(collective_id=1, has_side_effects=True, vmem_limit_bytes=67043328),
        cost_estimate=pl.CostEstimate(flops=2 * 10 ** 10, bytes_accessed=6 * w_act.size, transcendentals=0),
        name="moe",
    )(mixed, w_o, x_own, gain, w_router.T, choice, w_act, w_lin, down_t)


def rope_tables(lengths, steps, head):
    half = head // 2
    inv_freq = ROPE_BASE ** (-(jnp.arange(half, dtype=F32) * 2.0 / head))
    spots = (lengths[None, :] + jnp.arange(steps)[:, None]).reshape(-1).astype(F32)
    angles = spots[:, None] * inv_freq[None, :]
    return jnp.cos(angles), jnp.sin(angles)


def solution(mesh):
    x_count, y_count = mesh.shape['x'], mesh.shape['y']
    assert x_count == 4 and y_count == 4
    cache_spec = P('dp', None, 'y', None)
    in_specs = (P(None, 'dp'), P('dp'), P(None, 'dp', None), P(None, 'x'), cache_spec, cache_spec, P('x'), P('x', 'y'), P('x', 'y'), P('x', 'y'), P('y', 'x'), P('x'), P('x', None), P(None, 'x', 'y'), P(None, 'x', 'y'), P(None, 'y', 'x'))
    out_specs = (P(None, 'dp', 'x'), cache_spec, cache_spec)

    def per_device(tokens, lengths, choices, emb_table, k_cache, v_cache, g_attn, w_q, w_k, w_v, w_o, g_ffn, w_router, w_act, w_lin, w_down):
        steps, n_batch = tokens.shape
        heads, head = k_cache.shape[2], k_cache.shape[3]
        rows = steps * n_batch
        width_full = emb_table.shape[1] * x_count
        span = rows // y_count
        cos_t, sin_t = rope_tables(lengths, steps, head)
        x_own = gather(emb_table, tokens, span)
        kvq = qkv_sums(x_own, g_attn, w_q, w_k, w_v, rows, y_count, width_full)
        mixed, k_out, v_out = attention(lengths, kvq, cos_t, sin_t, k_cache, v_cache, steps)
        out = moe(mixed, w_o, x_own, g_ffn, w_router, jnp.transpose(choices, (0, 2, 1)), w_act, w_lin, w_down, y_count, width_full)
        return out.reshape(steps, n_batch, emb_table.shape[1]), k_out, v_out

    return jax.shard_map(per_device, mesh=mesh, in_specs=in_specs, out_specs=out_specs, check_vma=False)
```

```python
import functools
import jax
import jax.numpy as jnp
from jax import lax
from jax.experimental import pallas as pl
from jax.experimental.pallas import tpu as pltpu
from jax.sharding import PartitionSpec as P

EPS = 1e-5
ROPE_BASE = 1.0e6
F32 = jnp.float32
BF16 = jnp.bfloat16
LANES = 128


def dot(a, b):
    return lax.dot_general(a, b, (((1,), (0,)), ((), ())), preferred_element_type=F32)


def dot_nt(a, b):
    return lax.dot_general(a, b, (((1,), (1,)), ((), ())), preferred_element_type=F32)


def gather_kernel(span, vocab, depth, tok_ref, edge_ref, emb_ref, x_ref, buf, acc, sem):
    tiles = vocab // LANES
    batch = tok_ref.shape[1]
    start = lax.axis_index('y') * span

    def token(i):
        r = start + i
        return tok_ref[r // batch, lax.rem(r, batch)]

    def copy(i):
        tile = jnp.minimum(token(i) // LANES, tiles - 1)
        src = emb_ref.at[:, pl.ds(pl.multiple_of(tile * LANES, LANES), LANES)]
        slot = lax.rem(i, depth)
        return pltpu.make_async_copy(src, buf.at[slot], sem.at[slot])

    @pl.loop(0, min(depth, span))
    def _(i):
        copy(i).start()

    lane_id = lax.broadcasted_iota(jnp.int32, acc.shape, 1)

    @pl.loop(0, span)
    def _(i):
        copy(i).wait()
        tok = token(i)
        shift = lax.rem(i - lax.rem(tok, LANES) + LANES, LANES)
        edge = jnp.full(acc.shape, tok, jnp.int32) >= tiles * LANES
        moved = pltpu.roll(jnp.where(edge, edge_ref[...], buf[lax.rem(i, depth)]), shift, 1)
        acc[...] = jnp.where(lane_id == i, moved, acc[...])

        @pl.when(i + depth < span)
        def _():
            copy(i + depth).start()

    x_ref[...] = acc[...].astype(F32).T[:span].astype(BF16)


def gather(emb_table, tokens, span, depth=48):
    vocab, width = emb_table.shape
    table = emb_table.T
    return pl.pallas_call(
        functools.partial(gather_kernel, span, vocab, depth),
        grid=(1,),
        in_specs=[pl.BlockSpec(memory_space=pltpu.SMEM), pl.BlockSpec((width, LANES), lambda i: (0, vocab // LANES)), pl.BlockSpec(memory_space=pl.ANY)],
        out_specs=pl.BlockSpec((span, width), lambda i: (0, 0)),
        out_shape=jax.ShapeDtypeStruct((span, width), BF16),
        scratch_shapes=[pltpu.VMEM((depth, width, LANES), BF16), pltpu.VMEM((width, LANES), BF16), pltpu.SemaphoreType.DMA((depth,))],
        name="gather",
    )(tokens, table, table)


def attention_kernel(steps, batch, block, heads, head, lens_ref, kvq_ref, cos_ref, sin_ref, k_in, v_in, o_ref, k_out, v_out, q_rows, kt_ref, vt_ref, o_rows):
    cols = heads * head
    slots = k_in.shape[-1]
    rows = steps * batch
    i = pl.program_id(0)
    hpad = 16
    per_group = slots // 4

    @pl.when(i == 0)
    def _():
        def spread(table):
            four = jnp.concatenate([table] * (LANES // table.shape[1]), axis=1)
            return jnp.concatenate([four] * (cols // LANES) + [four[:, :cols % LANES]], axis=1)

        cosine, sine = spread(cos_ref[...]), spread(sin_ref[...])
        src = lax.broadcasted_iota(jnp.int32, (cols, cols), 0)
        dst = lax.broadcasted_iota(jnp.int32, (cols, cols), 1)
        low = dst % head < head // 2
        swap = jnp.where(low & (src == dst + head // 2), -1.0, jnp.where(~low & (src == dst - head // 2), 1.0, 0.0)).astype(BF16)
        row = lax.broadcasted_iota(jnp.int32, (rows, 4 * batch), 0)
        col = lax.broadcasted_iota(jnp.int32, (rows, 4 * batch), 1)
        perm = jnp.where((row // batch == col % 4) & (row % batch == col // 4), 1.0, 0.0).astype(BF16)
        for part in (2, 0):
            val = kvq_ref[part]
            swapped = dot(val, swap)
            rot = (val.astype(F32) * cosine + swapped * sine).astype(BF16).astype(F32)
            if part == 2:
                q_rows[...] = rot.reshape(steps, batch, cols)
            else:
                kt = dot(rot.T.astype(BF16), perm)
        vt = dot(kvq_ref[1].astype(F32).T.astype(BF16), perm)
        for g in range(batch // per_group):
            kt_ref[g] = kt[:, g * slots:(g + 1) * slots].astype(kt_ref.dtype)
            vt_ref[g] = vt[:, g * slots:(g + 1) * slots].astype(vt_ref.dtype)

    head_mask = lax.broadcasted_iota(jnp.int32, (hpad, cols), 1) // head == lax.broadcasted_iota(jnp.int32, (hpad, cols), 0)
    t_of = lax.broadcasted_iota(jnp.int32, (steps * hpad, slots), 0) // hpad
    s_of = lax.broadcasted_iota(jnp.int32, (steps * hpad, slots), 1)
    slot_id = lax.broadcasted_iota(jnp.int32, (cols, slots), 1)

    group = (i * block) // per_group
    news, scores_all = [], []
    for n in range(block):
        b = i * block + n
        first = lens_ref[b]
        shift = lax.rem(first - 4 * lax.rem(b, per_group) + slots, slots)
        fresh = (slot_id >= first) & (slot_id < first + steps)
        k_new = jnp.where(fresh, pltpu.roll(kt_ref[group], shift, 1).astype(BF16), k_in[n].reshape(cols, slots))
        v_new = jnp.where(fresh, pltpu.roll(vt_ref[group], shift, 1).astype(BF16), v_in[n].reshape(cols, slots))
        k_out[n] = k_new.reshape(heads, head, slots)
        v_out[n] = v_new.reshape(heads, head, slots)
        q_blk = jnp.concatenate([jnp.where(head_mask, jnp.broadcast_to(q_rows[t, pl.ds(b, 1), :], (hpad, cols)), 0.0) for t in range(steps)], axis=0).astype(BF16)
        scores = dot(q_blk, k_new) * head ** -0.5
        scores_all.append(jnp.where(s_of <= first + t_of, scores, -1.0e30))
        news.append(v_new)
    scores = jnp.concatenate(scores_all, axis=0)
    peak = jnp.max(scores, axis=-1, keepdims=True)
    weight = jnp.exp(scores - peak)
    inverse = 1.0 / jnp.sum(weight, axis=-1, keepdims=True)
    weight = weight.astype(BF16)
    span = steps * hpad
    for n in range(block):
        b = i * block + n
        mixed = dot_nt(weight[n * span:(n + 1) * span], news[n]) * inverse[n * span:(n + 1) * span]
        for t in range(steps):
            o_rows[t, pl.ds(b, 1), :] = jnp.sum(jnp.where(head_mask, mixed[t * hpad:(t + 1) * hpad], 0.0), axis=0, keepdims=True)

    @pl.when(i == pl.num_programs(0) - 1)
    def _():
        o_ref[...] = o_rows[...].reshape(rows, cols).astype(BF16)


def attention(lengths, kvq, cos_t, sin_t, k_cache, v_cache, steps, block=16, roll_dtype=BF16):
    batch, slots, heads, head = k_cache.shape
    cols, rows = heads * head, steps * batch
    k_t, v_t = jnp.transpose(k_cache, (0, 2, 3, 1)), jnp.transpose(v_cache, (0, 2, 3, 1))
    whole = lambda shape: pl.BlockSpec(shape, lambda i: (0,) * len(shape))
    cache_blk = pl.BlockSpec((block, heads, head, slots), lambda i: (i, 0, 0, 0))
    groups = 4 * batch // slots
    o, k_o, v_o = pl.pallas_call(
        functools.partial(attention_kernel, steps, batch, block, heads, head),
        grid=(batch // block,),
        in_specs=[pl.BlockSpec(memory_space=pltpu.SMEM), whole((3, rows, cols)), whole((rows, head // 2)), whole((rows, head // 2)), cache_blk, cache_blk],
        out_specs=[whole((rows, cols)), cache_blk, cache_blk],
        out_shape=[jax.ShapeDtypeStruct((rows, cols), BF16), jax.ShapeDtypeStruct(k_t.shape, BF16), jax.ShapeDtypeStruct(v_t.shape, BF16)],
        scratch_shapes=[pltpu.VMEM((steps, batch, cols), F32), pltpu.VMEM((groups, cols, slots), roll_dtype), pltpu.VMEM((groups, cols, slots), roll_dtype), pltpu.VMEM((steps, batch, cols), F32)],
        compiler_params=pltpu.CompilerParams(dimension_semantics=("arbitrary",)),
        cost_estimate=pl.CostEstimate(flops=4 * 10 ** 9, bytes_accessed=4 * k_t.size * 2, transcendentals=0),
        name="attention",
    )(lengths, kvq, cos_t, sin_t, k_t, v_t)
    back = lambda a: jnp.transpose(a, (0, 3, 1, 2))
    return o, back(k_o), back(v_o)


X, Y = 'x', 'y'
MESH = pl.DeviceIdType.MESH


def positions():
    xi, yi = lax.axis_index(X), lax.axis_index(Y)
    core, chip = lax.rem(xi, 2), xi // 2
    pair = xi + 1 - 2 * core
    cross = lax.rem(xi + 2, 4)
    diag = lax.rem(pair + 2, 4)
    return xi, yi, core, chip, pair, cross, diag


def knock(x_peers, yi, y_count):
    barrier = pltpu.get_barrier_semaphore()
    for peer in x_peers:
        pl.semaphore_signal(barrier, inc=1, device_id={X: peer}, device_id_type=MESH)
    for d in range(1, y_count):
        pl.semaphore_signal(barrier, inc=1, device_id={Y: lax.rem(yi + d, y_count)}, device_id_type=MESH)
    return lambda: pl.semaphore_wait(barrier, len(x_peers) + y_count - 1)


def remote(src, dst, send, recv, **where):
    return pltpu.make_async_remote_copy(src_ref=src, dst_ref=dst, send_sem=send, recv_sem=recv, device_id=where, device_id_type=MESH)


def start_all(copies):
    for c in copies:
        c.start()
    return copies


def scatter_y(src, dst, sems, yi, y_count, span):
    out = []
    for d in range(1, y_count):
        peer = lax.rem(yi + d, y_count)
        rows = pl.ds(pl.multiple_of(peer * span, span), span)
        out.append(remote(src.at[rows], dst.at[d - 1], sems.at[0, d - 1], sems.at[1, d - 1], y=peer))
    return start_all(out)


def gather_y(src, dst, sems, yi, y_count, span):
    rows = pl.ds(pl.multiple_of(yi * span, span), span)
    return start_all([remote(src, dst.at[rows], sems.at[0, d - 1], sems.at[1, d - 1], y=lax.rem(yi + d, y_count)) for d in range(1, y_count)])


def normalise(x_f32, gain, stat, stat_in, sems, peers, width_full, ready=None):
    rows = x_f32.shape[0]
    part = jnp.sum(x_f32 * x_f32, axis=-1, keepdims=True)
    stat[:, :rows] = jnp.broadcast_to(part, (rows, LANES)).T[:8]
    if ready:
        ready()
    copies = start_all([remote(stat, stat_in.at[i], sems.at[0, i], sems.at[1, i], x=peer) for i, peer in enumerate(peers)])
    for c in copies:
        c.wait()
    total = ((stat[...] + stat_in[0]) + (stat_in[1] + stat_in[2])).T[:rows, :1]
    return (x_f32 * lax.rsqrt(total / width_full + EPS) * gain).astype(BF16)


def qkv_kernel(y_count, width_full, x_ref, g_ref, wk_hbm, wv_hbm, wq_hbm, out_ref, weights, w_sem, stat, stat_in, h_own, h_all, keep, snd1, rcv1, snd2, rcv2, done, rcv3, stat_sem, y_sem, s1, s2, s3):
    xi, yi, core, chip, pair, cross, diag = positions()
    span, rows = x_ref.shape[0], h_all.shape[0]
    half = rows // 2
    ready = knock((pair, cross, diag), yi, y_count)
    loads = start_all([pltpu.make_async_copy(w, weights.at[m], w_sem.at[m]) for m, w in enumerate((wk_hbm, wv_hbm, wq_hbm))])
    stat[...] = jnp.zeros_like(stat)
    h = normalise(x_ref[...].astype(F32), g_ref[...].astype(F32)[None, :], stat, stat_in, stat_sem, (pair, cross, diag), width_full, ready)
    h_own[...] = h
    sent = gather_y(h_own, h_all, y_sem, yi, y_count, span)
    h_all[pl.ds(pl.multiple_of(yi * span, span), span)] = h
    for c in sent:
        c.wait()
    mine = pl.ds(pl.multiple_of(core * half, half), half)
    theirs = pl.ds(pl.multiple_of((1 - core) * half, half), half)
    first, second, third = [], [], []
    for m in range(3):
        loads[m].wait()
        snd1[m] = dot(h_all[theirs], weights[m]).astype(BF16)
        first += start_all([remote(snd1.at[m], rcv1.at[m], s1.at[0, m], s1.at[1, m], x=pair)])
        keep[m] = dot(h_all[mine], weights[m])
        first[m].wait_recv()
        snd2[m] = (keep[m] + rcv1[m].astype(F32)).astype(BF16)
        second += start_all([remote(snd2.at[m], rcv2.at[m], s2.at[0, m], s2.at[1, m], x=cross)])
    for m in range(3):
        second[m].wait_recv()
        done[m] = (snd2[m].astype(F32) + rcv2[m].astype(F32)).astype(BF16)
        third += start_all([remote(done.at[m], rcv3.at[m], s3.at[0, m], s3.at[1, m], x=pair)])
        out_ref[m, mine] = done[m]
    for m in range(3):
        third[m].wait_recv()
        out_ref[m, theirs] = rcv3[m]
    for c in first + second + third:
        c.wait_send()


def qkv_sums(x_own, gain, w_q, w_k, w_v, rows, y_count, width_full):
    span, width = x_own.shape
    cols, half = w_q.shape[1], rows // 2
    vmem = pl.BlockSpec(memory_space=pltpu.VMEM)
    part = pltpu.VMEM((3, half, cols), BF16)
    pairs = pltpu.SemaphoreType.DMA((2, 3))
    return pl.pallas_call(
        functools.partial(qkv_kernel, y_count, width_full),
        in_specs=[vmem] * 2 + [pl.BlockSpec(memory_space=pl.ANY)] * 3,
        out_specs=vmem,
        out_shape=jax.ShapeDtypeStruct((3, rows, cols), BF16),
        scratch_shapes=[pltpu.VMEM((3, width, cols), BF16), pltpu.SemaphoreType.DMA((3,)), pltpu.VMEM((8, LANES), F32), pltpu.VMEM((3, 8, LANES), F32), pltpu.VMEM((span, width), BF16), pltpu.VMEM((rows, width), BF16), pltpu.VMEM((3, half, cols), F32), part, part, part, part, part, part, pairs, pltpu.SemaphoreType.DMA((2, y_count - 1)), pairs, pairs, pairs],
        compiler_params=pltpu.CompilerParams(collective_id=0, has_side_effects=True),
        cost_estimate=pl.CostEstimate(flops=6 * rows * width * cols, bytes_accessed=8 * width * cols, transcendentals=0),
        name="qkv_sums",
    )(x_own, gain, w_k, w_v, w_q)


def chunks_of(ff, wide):
    return tuple((lo, min(wide, ff - lo)) for lo in range(0, ff, wide))


def moe_kernel(y_count, width_full, chunks, halves, experts, o_ref, wo_hbm, x_ref, g_ref, wr_ref, ch_ref, act_hbm, lin_hbm, down_hbm, out_ref, act, lin, down, stat, stat_in, part, rs_in, h_own, h_all, logit, logit_in, gate, mask, sparse, acc_down, x_mid, wo, wo_sem, *rest):
    n_chunk = len(chunks)
    keep, snd1, rcv1, snd2, rcv2, u_mine, u_pair = [rest[i * n_chunk:(i + 1) * n_chunk] for i in range(7)]
    last = rest[7 * n_chunk:7 * n_chunk + 8]
    part2, rs2_in, own2, all2 = last[:2], last[2:4], last[4:6], last[6:]
    w_sem, stat_sem, rs_sem, ag_sem, lg_sem, s1, s2, s3, s4, s5, rs2_sem, ag2_sem = rest[7 * n_chunk + 8:]
    xi, yi, core, chip, pair, cross, diag = positions()
    peers = (pair, cross, diag)
    span, rows = x_ref.shape[0], h_all.shape[0]
    half, width = rows // 2, x_ref.shape[1]
    ready = knock(peers, yi, y_count)
    wo_load = pltpu.make_async_copy(wo_hbm, wo, wo_sem)
    wo_load.start()
    loads = []
    for i, (src, dst) in enumerate(((act_hbm, act), (lin_hbm, lin), (down_hbm, down))):
        for e in range(experts):
            place = dst.at[e] if i == 2 else dst.at[pl.ds(e * width, width)]
            loads.append(pltpu.make_async_copy(src.at[e], place, w_sem.at[i, e]))
    start_all(loads)
    stat[...] = jnp.zeros_like(stat)
    logit[...] = jnp.zeros_like(logit)
    own = pl.ds(pl.multiple_of(yi * span, span), span)
    wo_load.wait()
    part[...] = dot(o_ref[...], wo[...]).astype(BF16)
    ch = ch_ref[...].astype(F32)
    ch = jnp.concatenate([jnp.concatenate([ch[t], jnp.zeros((8 - ch.shape[1], ch.shape[2]), F32)], axis=0).T for t in range(ch.shape[0])], axis=0)
    ch_keep = jnp.where(core == 0, ch[:, :1], ch[:, 1:2])
    ch_send = jnp.where(core == 0, ch[:, 1:2], ch[:, :1])
    for e in range(experts):
        mask[0, e] = jnp.broadcast_to(jnp.where(ch_keep == e, 1.0, 0.0), (rows, LANES)).astype(BF16)
        mask[1, e] = jnp.broadcast_to(jnp.where(ch_send == e, 1.0, 0.0), (rows, LANES)).astype(BF16)

    ready()
    sent = scatter_y(part, rs_in, rs_sem, yi, y_count, span)

    def wide_mask(s, e, n):
        return jnp.concatenate([mask[s, e]] * (n // LANES) + ([mask[s, e][:, :n % LANES]] if n % LANES else []), axis=1)

    for c in sent:
        c.wait()
    total = part[own].astype(F32) + rs_in[0].astype(F32) + rs_in[1].astype(F32) + rs_in[2].astype(F32)
    x_new = (x_ref[...].astype(F32) + total).astype(BF16)
    x_mid[...] = x_new
    h = normalise(x_new.astype(F32), g_ref[...].astype(F32)[None, :], stat, stat_in, stat_sem, peers, width_full)
    h_own[...] = h
    sent = gather_y(h_own, h_all, ag_sem, yi, y_count, span)
    h_all[own] = h
    for c in sent:
        c.wait()
    logit[:, :rows] = dot_nt(wr_ref[...], h_all[...])
    lg = start_all([remote(logit, logit_in.at[i], lg_sem.at[0, i], lg_sem.at[1, i], x=peer) for i, peer in enumerate(peers)])
    h2 = h_all[...]
    for e in range(experts):
        for s in range(2):
            sparse[s, :, e * width:(e + 1) * width] = h2 * wide_mask(s, e, width)

    for copy in loads[:2 * experts]:
        copy.wait()

    mine = pl.ds(pl.multiple_of(chip * half, half), half)
    other = pl.ds(pl.multiple_of((1 - chip) * half, half), half)
    first, second, to_cross, to_pair, forward = [], [], [], [], []

    def product(s, w, lo, n):
        return dot(sparse[s], w[:, lo:lo + n])

    def sums(k):
        lo, n = chunks[k]
        snd1[k][0] = product(1, act, lo, n).astype(BF16)
        snd1[k][1] = product(1, lin, lo, n).astype(BF16)
        first.extend(start_all([remote(snd1[k], rcv1[k], s1.at[0, k], s1.at[1, k], x=pair)]))
        keep[k][0] = product(0, act, lo, n)
        keep[k][1] = product(0, lin, lo, n)
        first[k].wait_recv()
        for i in range(2):
            snd2[k][i] = (keep[k][i, other] + rcv1[k][i, other].astype(F32)).astype(BF16)
        second.extend(start_all([remote(snd2[k], rcv2[k], s2.at[0, k], s2.at[1, k], x=cross)]))
        for i in range(2):
            keep[k][i, mine] = keep[k][i, mine] + rcv1[k][i, mine].astype(F32)

    def gates():
        for c in lg:
            c.wait()
        logits = ((logit[...] + logit_in[0]) + (logit_in[1] + logit_in[2])).T[:rows]
        col = lax.broadcasted_iota(jnp.int32, logits.shape, 1).astype(F32)
        l_keep = jnp.sum(jnp.where(col == ch_keep, logits, 0.0), axis=1, keepdims=True)
        l_send = jnp.sum(jnp.where(col == ch_send, logits, 0.0), axis=1, keepdims=True)
        top = jnp.maximum(l_keep, l_send)
        e_keep, e_send = jnp.exp(l_keep - top), jnp.exp(l_send - top)
        gate[...] = jnp.broadcast_to(e_keep / (e_keep + e_send), gate.shape)

    def unit(k):
        second[k].wait_recv()
        a = keep[k][0, mine] + rcv2[k][0].astype(F32)
        b = keep[k][1, mine] + rcv2[k][1].astype(F32)
        u_mine[k][mine] = (gate[mine][:, :1] * (a * jax.nn.sigmoid(a)) * b).astype(BF16)
        to_cross.extend(start_all([remote(u_mine[k].at[mine], u_mine[k].at[mine], s3.at[0, k], s3.at[1, k], x=cross)]))
        to_pair.extend(start_all([remote(u_mine[k].at[mine], u_pair[k].at[mine], s4.at[0, k], s4.at[1, k], x=pair)]))

    def pass_on(k):
        to_cross[k].wait_recv()
        forward.extend(start_all([remote(u_mine[k].at[other], u_pair[k].at[other], s5.at[0, k], s5.at[1, k], x=pair)]))

    def downward(k):
        lo, n = chunks[k]
        to_pair[k].wait_recv()
        forward[k].wait_recv()
        u0, u1 = u_mine[k][...], u_pair[k][...]
        total = jnp.zeros((width, rows), F32) if k == 0 else acc_down[...]
        for e in range(experts):
            total = total + dot_nt(down[e, :, lo:lo + n], u0 * wide_mask(0, e, n) + u1 * wide_mask(1, e, n))
        acc_down[...] = total

    sums(0)
    sums(1)
    gates()
    sums(2)
    for k in range(3, n_chunk):
        unit(k - 3)
        sums(k)
        if k > 3:
            pass_on(k - 4)
    for copy in loads[2 * experts:]:
        copy.wait()
    unit(n_chunk - 3)
    downward(0)
    unit(n_chunk - 2)
    downward(1)
    pass_on(n_chunk - 4)
    unit(n_chunk - 1)
    pass_on(n_chunk - 3)
    for k in range(2, n_chunk - 3):
        downward(k)
    pass_on(n_chunk - 2)
    downward(n_chunk - 3)
    pass_on(n_chunk - 1)
    downward(n_chunk - 2)
    downward(n_chunk - 1)

    sums2, copies2 = [], []
    for i, (lo, n) in enumerate(halves):
        part2[i][...] = acc_down[lo:lo + n].T.astype(BF16)
        sums2.append(scatter_y(part2[i], rs2_in[i], rs2_sem.at[i], yi, y_count, span))
    for i, (lo, n) in enumerate(halves):
        for c in sums2[i]:
            c.wait()
        total = part2[i][own].astype(F32) + rs2_in[i][0].astype(F32) + rs2_in[i][1].astype(F32) + rs2_in[i][2].astype(F32)
        h_new = (x_mid[:, lo:lo + n].astype(F32) + total).astype(BF16)
        own2[i][...] = h_new
        copies2.append(gather_y(own2[i], all2[i], ag2_sem.at[i], yi, y_count, span))
        all2[i][own] = h_new
    for i, (lo, n) in enumerate(halves):
        for c in copies2[i]:
            c.wait()
        out_ref[:, lo:lo + n] = all2[i][...]
    for c in first + second + to_cross + to_pair + forward:
        c.wait_send()


def moe(mixed, w_o, x_own, gain, w_router, choice, w_act, w_lin, w_down, y_count, width_full):
    rows, heads = mixed.shape
    span, width = x_own.shape
    experts, _, ff = w_act.shape
    half, chunks = rows // 2, chunks_of(ff, 256)
    halves = ((0, 256), (256, width - 256))
    vmem, hbm = pl.BlockSpec(memory_space=pltpu.VMEM), pl.BlockSpec(memory_space=pl.ANY)
    down_t = jnp.transpose(w_down, (0, 2, 1))
    three = pltpu.SemaphoreType.DMA((2, 3))
    ring = pltpu.SemaphoreType.DMA((2, y_count - 1))
    per_chunk = pltpu.SemaphoreType.DMA((2, len(chunks)))
    buf = lambda lead, r, dt: [pltpu.VMEM(lead + (r, n), dt) for _, n in chunks]
    flat = (experts * width, ff)
    scratch = [pltpu.VMEM(flat, BF16), pltpu.VMEM(flat, BF16), pltpu.VMEM(down_t.shape, BF16), pltpu.VMEM((8, LANES), F32), pltpu.VMEM((3, 8, LANES), F32), pltpu.VMEM((rows, width), BF16), pltpu.VMEM((y_count - 1, span, width), BF16), pltpu.VMEM((span, width), BF16), pltpu.VMEM((rows, width), BF16), pltpu.VMEM((experts, 2 * LANES), F32), pltpu.VMEM((3, experts, 2 * LANES), F32), pltpu.VMEM((rows, LANES), F32), pltpu.VMEM((2, experts, rows, LANES), BF16), pltpu.VMEM((2, rows, experts * width), BF16), pltpu.VMEM((width, rows), F32), pltpu.VMEM((span, width), BF16), pltpu.VMEM(w_o.shape, BF16), pltpu.SemaphoreType.DMA]
    scratch += buf((2,), rows, F32) + buf((2,), rows, BF16) + buf((2,), rows, BF16) + buf((2,), half, BF16) + buf((2,), half, BF16) + buf((), rows, BF16) + buf((), rows, BF16)
    for lead, r in (((), rows), ((y_count - 1,), span), ((), span), ((), rows)):
        scratch += [pltpu.VMEM(lead + (r, n), BF16) for _, n in halves]
    rings = pltpu.SemaphoreType.DMA((2, 2, y_count - 1))
    scratch += [pltpu.SemaphoreType.DMA((3, experts)), three, ring, ring, three] + [per_chunk] * 5 + [rings, rings]
    return pl.pallas_call(
        functools.partial(moe_kernel, y_count, width_full, chunks, halves, experts),
        in_specs=[vmem, hbm] + [vmem] * 4 + [hbm] * 3,
        out_specs=vmem,
        out_shape=jax.ShapeDtypeStruct((rows, width), BF16),
        scratch_shapes=scratch,
        compiler_params=pltpu.CompilerParams(collective_id=1, has_side_effects=True, vmem_limit_bytes=67043328),
        cost_estimate=pl.CostEstimate(flops=2 * 10 ** 10, bytes_accessed=6 * w_act.size, transcendentals=0),
        name="moe",
    )(mixed, w_o, x_own, gain, w_router.T, choice, w_act, w_lin, down_t)


def rope_tables(lengths, steps, head):
    half = head // 2
    inv_freq = ROPE_BASE ** (-(jnp.arange(half, dtype=F32) * 2.0 / head))
    spots = (lengths[None, :] + jnp.arange(steps)[:, None]).reshape(-1).astype(F32)
    angles = spots[:, None] * inv_freq[None, :]
    return jnp.cos(angles), jnp.sin(angles)


def solution(mesh):
    x_count, y_count = mesh.shape['x'], mesh.shape['y']
    assert x_count == 4 and y_count == 4
    cache_spec = P('dp', None, 'y', None)
    in_specs = (P(None, 'dp'), P('dp'), P(None, 'dp', None), P(None, 'x'), cache_spec, cache_spec, P('x'), P('x', 'y'), P('x', 'y'), P('x', 'y'), P('y', 'x'), P('x'), P('x', None), P(None, 'x', 'y'), P(None, 'x', 'y'), P(None, 'y', 'x'))
    out_specs = (P(None, 'dp', 'x'), cache_spec, cache_spec)

    def per_device(tokens, lengths, choices, emb_table, k_cache, v_cache, g_attn, w_q, w_k, w_v, w_o, g_ffn, w_router, w_act, w_lin, w_down):
        steps, n_batch = tokens.shape
        heads, head = k_cache.shape[2], k_cache.shape[3]
        rows = steps * n_batch
        width_full = emb_table.shape[1] * x_count
        span = rows // y_count
        cos_t, sin_t = rope_tables(lengths, steps, head)
        x_own = gather(emb_table, tokens, span)
        kvq = qkv_sums(x_own, g_attn, w_q, w_k, w_v, rows, y_count, width_full)
        mixed, k_out, v_out = attention(lengths, kvq, cos_t, sin_t, k_cache, v_cache, steps)
        out = moe(mixed, w_o, x_own, g_ffn, w_router, jnp.transpose(choices, (0, 2, 1)), w_act, w_lin, w_down, y_count, width_full)
        return out.reshape(steps, n_batch, emb_table.shape[1]), k_out, v_out

    return jax.shard_map(per_device, mesh=mesh, in_specs=in_specs, out_specs=out_specs, check_vma=False)
```

```python
import functools
import jax
import jax.numpy as jnp
from jax import lax
from jax.experimental import pallas as pl
from jax.experimental.pallas import tpu as pltpu
from jax.sharding import PartitionSpec as P

EPS = 1e-5
ROPE_BASE = 1.0e6
F32 = jnp.float32
BF16 = jnp.bfloat16
LANES = 128


def dot(a, b):
    return lax.dot_general(a, b, (((1,), (0,)), ((), ())), preferred_element_type=F32)


def dot_nt(a, b):
    return lax.dot_general(a, b, (((1,), (1,)), ((), ())), preferred_element_type=F32)


def gather_kernel(span, vocab, depth, tok_ref, edge_ref, emb_ref, x_ref, buf, acc, sem):
    tiles = vocab // LANES
    batch = tok_ref.shape[1]
    start = lax.axis_index('y') * span

    def token(i):
        r = start + i
        return tok_ref[r // batch, lax.rem(r, batch)]

    def copy(i):
        tile = jnp.minimum(token(i) // LANES, tiles - 1)
        src = emb_ref.at[:, pl.ds(pl.multiple_of(tile * LANES, LANES), LANES)]
        slot = lax.rem(i, depth)
        return pltpu.make_async_copy(src, buf.at[slot], sem.at[slot])

    @pl.loop(0, min(depth, span))
    def _(i):
        copy(i).start()

    lane_id = lax.broadcasted_iota(jnp.int32, acc.shape, 1)

    @pl.loop(0, span)
    def _(i):
        copy(i).wait()
        tok = token(i)
        shift = lax.rem(i - lax.rem(tok, LANES) + LANES, LANES)
        edge = jnp.full(acc.shape, tok, jnp.int32) >= tiles * LANES
        moved = pltpu.roll(jnp.where(edge, edge_ref[...], buf[lax.rem(i, depth)]), shift, 1)
        acc[...] = jnp.where(lane_id == i, moved, acc[...])

        @pl.when(i + depth < span)
        def _():
            copy(i + depth).start()

    x_ref[...] = acc[...].astype(F32).T[:span].astype(BF16)


def gather(emb_table, tokens, span, depth=48):
    vocab, width = emb_table.shape
    table = emb_table.T
    return pl.pallas_call(
        functools.partial(gather_kernel, span, vocab, depth),
        grid=(1,),
        in_specs=[pl.BlockSpec(memory_space=pltpu.SMEM), pl.BlockSpec((width, LANES), lambda i: (0, vocab // LANES)), pl.BlockSpec(memory_space=pl.ANY)],
        out_specs=pl.BlockSpec((span, width), lambda i: (0, 0)),
        out_shape=jax.ShapeDtypeStruct((span, width), BF16),
        scratch_shapes=[pltpu.VMEM((depth, width, LANES), BF16), pltpu.VMEM((width, LANES), BF16), pltpu.SemaphoreType.DMA((depth,))],
        name="gather",
    )(tokens, table, table)


def attention_kernel(steps, batch, block, heads, head, lens_ref, kvq_ref, cos_ref, sin_ref, k_in, v_in, o_ref, k_out, v_out, q_rows, kt_ref, vt_ref, o_rows):
    cols = heads * head
    slots = k_in.shape[-1]
    rows = steps * batch
    i = pl.program_id(0)
    hpad = 16
    per_group = slots // 4

    @pl.when(i == 0)
    def _():
        def spread(table):
            four = jnp.concatenate([table] * (LANES // table.shape[1]), axis=1)
            return jnp.concatenate([four] * (cols // LANES) + [four[:, :cols % LANES]], axis=1)

        cosine, sine = spread(cos_ref[...]), spread(sin_ref[...])
        src = lax.broadcasted_iota(jnp.int32, (cols, cols), 0)
        dst = lax.broadcasted_iota(jnp.int32, (cols, cols), 1)
        low = dst % head < head // 2
        swap = jnp.where(low & (src == dst + head // 2), -1.0, jnp.where(~low & (src == dst - head // 2), 1.0, 0.0)).astype(BF16)
        row = lax.broadcasted_iota(jnp.int32, (rows, 4 * batch), 0)
        col = lax.broadcasted_iota(jnp.int32, (rows, 4 * batch), 1)
        perm = jnp.where((row // batch == col % 4) & (row % batch == col // 4), 1.0, 0.0).astype(BF16)
        for part in (2, 0):
            val = kvq_ref[part]
            swapped = dot(val, swap)
            rot = (val.astype(F32) * cosine + swapped * sine).astype(BF16).astype(F32)
            if part == 2:
                q_rows[...] = rot.reshape(steps, batch, cols)
            else:
                kt = dot(rot.T.astype(BF16), perm)
        vt = dot(kvq_ref[1].astype(F32).T.astype(BF16), perm)
        for g in range(batch // per_group):
            kt_ref[g] = kt[:, g * slots:(g + 1) * slots].astype(kt_ref.dtype)
            vt_ref[g] = vt[:, g * slots:(g + 1) * slots].astype(vt_ref.dtype)

    head_mask = lax.broadcasted_iota(jnp.int32, (hpad, cols), 1) // head == lax.broadcasted_iota(jnp.int32, (hpad, cols), 0)
    t_of = lax.broadcasted_iota(jnp.int32, (steps * hpad, slots), 0) // hpad
    s_of = lax.broadcasted_iota(jnp.int32, (steps * hpad, slots), 1)
    slot_id = lax.broadcasted_iota(jnp.int32, (cols, slots), 1)

    group = (i * block) // per_group
    news, scores_all = [], []
    for n in range(block):
        b = i * block + n
        first = lens_ref[b]
        shift = lax.rem(first - 4 * lax.rem(b, per_group) + slots, slots)
        fresh = (slot_id >= first) & (slot_id < first + steps)
        k_new = jnp.where(fresh, pltpu.roll(kt_ref[group], shift, 1).astype(BF16), k_in[n].reshape(cols, slots))
        v_new = jnp.where(fresh, pltpu.roll(vt_ref[group], shift, 1).astype(BF16), v_in[n].reshape(cols, slots))
        k_out[n] = k_new.reshape(heads, head, slots)
        v_out[n] = v_new.reshape(heads, head, slots)
        q_blk = jnp.concatenate([jnp.where(head_mask, jnp.broadcast_to(q_rows[t, pl.ds(b, 1), :], (hpad, cols)), 0.0) for t in range(steps)], axis=0).astype(BF16)
        scores = dot(q_blk, k_new) * head ** -0.5
        scores_all.append(jnp.where(s_of <= first + t_of, scores, -1.0e30))
        news.append(v_new)
    scores = jnp.concatenate(scores_all, axis=0)
    peak = jnp.max(scores, axis=-1, keepdims=True)
    weight = jnp.exp(scores - peak)
    inverse = 1.0 / jnp.sum(weight, axis=-1, keepdims=True)
    weight = weight.astype(BF16)
    span = steps * hpad
    for n in range(block):
        b = i * block + n
        mixed = dot_nt(weight[n * span:(n + 1) * span], news[n]) * inverse[n * span:(n + 1) * span]
        for t in range(steps):
            o_rows[t, pl.ds(b, 1), :] = jnp.sum(jnp.where(head_mask, mixed[t * hpad:(t + 1) * hpad], 0.0), axis=0, keepdims=True)

    @pl.when(i == pl.num_programs(0) - 1)
    def _():
        o_ref[...] = o_rows[...].reshape(rows, cols).astype(BF16)


def attention(lengths, kvq, cos_t, sin_t, k_cache, v_cache, steps, block=16, roll_dtype=BF16):
    batch, slots, heads, head = k_cache.shape
    cols, rows = heads * head, steps * batch
    k_t, v_t = jnp.transpose(k_cache, (0, 2, 3, 1)), jnp.transpose(v_cache, (0, 2, 3, 1))
    whole = lambda shape: pl.BlockSpec(shape, lambda i: (0,) * len(shape))
    cache_blk = pl.BlockSpec((block, heads, head, slots), lambda i: (i, 0, 0, 0))
    groups = 4 * batch // slots
    o, k_o, v_o = pl.pallas_call(
        functools.partial(attention_kernel, steps, batch, block, heads, head),
        grid=(batch // block,),
        in_specs=[pl.BlockSpec(memory_space=pltpu.SMEM), whole((3, rows, cols)), whole((rows, head // 2)), whole((rows, head // 2)), cache_blk, cache_blk],
        out_specs=[whole((rows, cols)), cache_blk, cache_blk],
        out_shape=[jax.ShapeDtypeStruct((rows, cols), BF16), jax.ShapeDtypeStruct(k_t.shape, BF16), jax.ShapeDtypeStruct(v_t.shape, BF16)],
        scratch_shapes=[pltpu.VMEM((steps, batch, cols), F32), pltpu.VMEM((groups, cols, slots), roll_dtype), pltpu.VMEM((groups, cols, slots), roll_dtype), pltpu.VMEM((steps, batch, cols), F32)],
        compiler_params=pltpu.CompilerParams(dimension_semantics=("arbitrary",)),
        cost_estimate=pl.CostEstimate(flops=4 * 10 ** 9, bytes_accessed=4 * k_t.size * 2, transcendentals=0),
        name="attention",
    )(lengths, kvq, cos_t, sin_t, k_t, v_t)
    back = lambda a: jnp.transpose(a, (0, 3, 1, 2))
    return o, back(k_o), back(v_o)


X, Y = 'x', 'y'
MESH = pl.DeviceIdType.MESH


def positions():
    xi, yi = lax.axis_index(X), lax.axis_index(Y)
    core, chip = lax.rem(xi, 2), xi // 2
    pair = xi + 1 - 2 * core
    cross = lax.rem(xi + 2, 4)
    diag = lax.rem(pair + 2, 4)
    return xi, yi, core, chip, pair, cross, diag


def knock(x_peers, yi, y_count):
    barrier = pltpu.get_barrier_semaphore()
    for peer in x_peers:
        pl.semaphore_signal(barrier, inc=1, device_id={X: peer}, device_id_type=MESH)
    for d in range(1, y_count):
        pl.semaphore_signal(barrier, inc=1, device_id={Y: lax.rem(yi + d, y_count)}, device_id_type=MESH)
    return lambda: pl.semaphore_wait(barrier, len(x_peers) + y_count - 1)


def remote(src, dst, send, recv, **where):
    return pltpu.make_async_remote_copy(src_ref=src, dst_ref=dst, send_sem=send, recv_sem=recv, device_id=where, device_id_type=MESH)


def start_all(copies):
    for c in copies:
        c.start()
    return copies


def scatter_y(src, dst, sems, yi, y_count, span):
    out = []
    for d in range(1, y_count):
        peer = lax.rem(yi + d, y_count)
        rows = pl.ds(pl.multiple_of(peer * span, span), span)
        out.append(remote(src.at[rows], dst.at[d - 1], sems.at[0, d - 1], sems.at[1, d - 1], y=peer))
    return start_all(out)


def gather_y(src, dst, sems, yi, y_count, span):
    rows = pl.ds(pl.multiple_of(yi * span, span), span)
    return start_all([remote(src, dst.at[rows], sems.at[0, d - 1], sems.at[1, d - 1], y=lax.rem(yi + d, y_count)) for d in range(1, y_count)])


def normalise(x_f32, gain, stat, stat_in, sems, peers, width_full, ready=None):
    rows = x_f32.shape[0]
    part = jnp.sum(x_f32 * x_f32, axis=-1, keepdims=True)
    stat[:, :rows] = jnp.broadcast_to(part, (rows, LANES)).T[:8]
    if ready:
        ready()
    copies = start_all([remote(stat, stat_in.at[i], sems.at[0, i], sems.at[1, i], x=peer) for i, peer in enumerate(peers)])
    for c in copies:
        c.wait()
    total = ((stat[...] + stat_in[0]) + (stat_in[1] + stat_in[2])).T[:rows, :1]
    return (x_f32 * lax.rsqrt(total / width_full + EPS) * gain).astype(BF16)


def qkv_kernel(y_count, width_full, x_ref, g_ref, wk_hbm, wv_hbm, wq_hbm, out_ref, weights, w_sem, stat, stat_in, h_own, h_all, keep, snd1, rcv1, snd2, rcv2, done, rcv3, stat_sem, y_sem, s1, s2, s3):
    xi, yi, core, chip, pair, cross, diag = positions()
    span, rows = x_ref.shape[0], h_all.shape[0]
    half = rows // 2
    ready = knock((pair, cross, diag), yi, y_count)
    loads = start_all([pltpu.make_async_copy(w, weights.at[m], w_sem.at[m]) for m, w in enumerate((wk_hbm, wv_hbm, wq_hbm))])
    stat[...] = jnp.zeros_like(stat)
    h = normalise(x_ref[...].astype(F32), g_ref[...].astype(F32)[None, :], stat, stat_in, stat_sem, (pair, cross, diag), width_full, ready)
    h_own[...] = h
    sent = gather_y(h_own, h_all, y_sem, yi, y_count, span)
    h_all[pl.ds(pl.multiple_of(yi * span, span), span)] = h
    for c in sent:
        c.wait()
    mine = pl.ds(pl.multiple_of(core * half, half), half)
    theirs = pl.ds(pl.multiple_of((1 - core) * half, half), half)
    first, second, third = [], [], []
    for m in range(3):
        loads[m].wait()
        snd1[m] = dot(h_all[theirs], weights[m]).astype(BF16)
        first += start_all([remote(snd1.at[m], rcv1.at[m], s1.at[0, m], s1.at[1, m], x=pair)])
        keep[m] = dot(h_all[mine], weights[m])
        first[m].wait_recv()
        snd2[m] = (keep[m] + rcv1[m].astype(F32)).astype(BF16)
        second += start_all([remote(snd2.at[m], rcv2.at[m], s2.at[0, m], s2.at[1, m], x=cross)])
    for m in range(3):
        second[m].wait_recv()
        done[m] = (snd2[m].astype(F32) + rcv2[m].astype(F32)).astype(BF16)
        third += start_all([remote(done.at[m], rcv3.at[m], s3.at[0, m], s3.at[1, m], x=pair)])
        out_ref[m, mine] = done[m]
    for m in range(3):
        third[m].wait_recv()
        out_ref[m, theirs] = rcv3[m]
    for c in first + second + third:
        c.wait_send()


def qkv_sums(x_own, gain, w_q, w_k, w_v, rows, y_count, width_full):
    span, width = x_own.shape
    cols, half = w_q.shape[1], rows // 2
    vmem = pl.BlockSpec(memory_space=pltpu.VMEM)
    part = pltpu.VMEM((3, half, cols), BF16)
    pairs = pltpu.SemaphoreType.DMA((2, 3))
    return pl.pallas_call(
        functools.partial(qkv_kernel, y_count, width_full),
        in_specs=[vmem] * 2 + [pl.BlockSpec(memory_space=pl.ANY)] * 3,
        out_specs=vmem,
        out_shape=jax.ShapeDtypeStruct((3, rows, cols), BF16),
        scratch_shapes=[pltpu.VMEM((3, width, cols), BF16), pltpu.SemaphoreType.DMA((3,)), pltpu.VMEM((8, LANES), F32), pltpu.VMEM((3, 8, LANES), F32), pltpu.VMEM((span, width), BF16), pltpu.VMEM((rows, width), BF16), pltpu.VMEM((3, half, cols), F32), part, part, part, part, part, part, pairs, pltpu.SemaphoreType.DMA((2, y_count - 1)), pairs, pairs, pairs],
        compiler_params=pltpu.CompilerParams(collective_id=0, has_side_effects=True),
        cost_estimate=pl.CostEstimate(flops=6 * rows * width * cols, bytes_accessed=8 * width * cols, transcendentals=0),
        name="qkv_sums",
    )(x_own, gain, w_k, w_v, w_q)


def chunks_of(ff, wide):
    return tuple((lo, min(wide, ff - lo)) for lo in range(0, ff, wide))


def moe_kernel(y_count, width_full, chunks, halves, experts, o_ref, wo_hbm, x_ref, g_ref, wr_ref, ch_ref, act_hbm, lin_hbm, down_hbm, out_ref, act, lin, down, stat, stat_in, part, rs_in, h_own, h_all, logit, logit_in, gate, mask, sparse, acc_down, x_mid, wo, wo_sem, *rest):
    n_chunk = len(chunks)
    keep, snd1, rcv1, snd2, rcv2, u_mine, u_pair = [rest[i * n_chunk:(i + 1) * n_chunk] for i in range(7)]
    last = rest[7 * n_chunk:7 * n_chunk + 8]
    part2, rs2_in, own2, all2 = last[:2], last[2:4], last[4:6], last[6:]
    w_sem, stat_sem, rs_sem, ag_sem, lg_sem, s1, s2, s3, s4, s5, rs2_sem, ag2_sem = rest[7 * n_chunk + 8:]
    xi, yi, core, chip, pair, cross, diag = positions()
    peers = (pair, cross, diag)
    span, rows = x_ref.shape[0], h_all.shape[0]
    half, width = rows // 2, x_ref.shape[1]
    ready = knock(peers, yi, y_count)
    wo_load = pltpu.make_async_copy(wo_hbm, wo, wo_sem)
    wo_load.start()
    loads = []
    for i, (src, dst) in enumerate(((act_hbm, act), (lin_hbm, lin), (down_hbm, down))):
        for e in range(experts):
            place = dst.at[e] if i == 2 else dst.at[pl.ds(e * width, width)]
            loads.append(pltpu.make_async_copy(src.at[e], place, w_sem.at[i, e]))
    start_all(loads)
    stat[...] = jnp.zeros_like(stat)
    logit[...] = jnp.zeros_like(logit)
    own = pl.ds(pl.multiple_of(yi * span, span), span)
    wo_load.wait()
    part[...] = dot(o_ref[...], wo[...]).astype(BF16)
    ch = ch_ref[...].astype(F32)
    ch = jnp.concatenate([jnp.concatenate([ch[t], jnp.zeros((8 - ch.shape[1], ch.shape[2]), F32)], axis=0).T for t in range(ch.shape[0])], axis=0)
    ch_keep = jnp.where(core == 0, ch[:, :1], ch[:, 1:2])
    ch_send = jnp.where(core == 0, ch[:, 1:2], ch[:, :1])
    for e in range(experts):
        mask[0, e] = jnp.broadcast_to(jnp.where(ch_keep == e, 1.0, 0.0), (rows, LANES)).astype(BF16)
        mask[1, e] = jnp.broadcast_to(jnp.where(ch_send == e, 1.0, 0.0), (rows, LANES)).astype(BF16)

    ready()
    sent = scatter_y(part, rs_in, rs_sem, yi, y_count, span)

    def wide_mask(s, e, n):
        return jnp.concatenate([mask[s, e]] * (n // LANES) + ([mask[s, e][:, :n % LANES]] if n % LANES else []), axis=1)

    for c in sent:
        c.wait()
    total = part[own].astype(F32) + rs_in[0].astype(F32) + rs_in[1].astype(F32) + rs_in[2].astype(F32)
    x_new = (x_ref[...].astype(F32) + total).astype(BF16)
    x_mid[...] = x_new
    h = normalise(x_new.astype(F32), g_ref[...].astype(F32)[None, :], stat, stat_in, stat_sem, peers, width_full)
    h_own[...] = h
    sent = gather_y(h_own, h_all, ag_sem, yi, y_count, span)
    h_all[own] = h
    for c in sent:
        c.wait()
    logit[:, :rows] = dot_nt(wr_ref[...], h_all[...])
    lg = start_all([remote(logit, logit_in.at[i], lg_sem.at[0, i], lg_sem.at[1, i], x=peer) for i, peer in enumerate(peers)])
    h2 = h_all[...]
    for e in range(experts):
        for s in range(2):
            sparse[s, :, e * width:(e + 1) * width] = h2 * wide_mask(s, e, width)

    for copy in loads[:2 * experts]:
        copy.wait()

    mine = pl.ds(pl.multiple_of(chip * half, half), half)
    other = pl.ds(pl.multiple_of((1 - chip) * half, half), half)
    first, second, to_cross, to_pair, forward = [], [], [], [], []

    def product(s, w, lo, n):
        return dot(sparse[s], w[:, lo:lo + n])

    def sums(k):
        lo, n = chunks[k]
        snd1[k][0] = product(1, act, lo, n).astype(BF16)
        snd1[k][1] = product(1, lin, lo, n).astype(BF16)
        first.extend(start_all([remote(snd1[k], rcv1[k], s1.at[0, k], s1.at[1, k], x=pair)]))
        keep[k][0] = product(0, act, lo, n)
        keep[k][1] = product(0, lin, lo, n)
        first[k].wait_recv()
        for i in range(2):
            snd2[k][i] = (keep[k][i, other] + rcv1[k][i, other].astype(F32)).astype(BF16)
        second.extend(start_all([remote(snd2[k], rcv2[k], s2.at[0, k], s2.at[1, k], x=cross)]))
        for i in range(2):
            keep[k][i, mine] = keep[k][i, mine] + rcv1[k][i, mine].astype(F32)

    def gates():
        for c in lg:
            c.wait()
        logits = ((logit[...] + logit_in[0]) + (logit_in[1] + logit_in[2])).T[:rows]
        col = lax.broadcasted_iota(jnp.int32, logits.shape, 1).astype(F32)
        l_keep = jnp.sum(jnp.where(col == ch_keep, logits, 0.0), axis=1, keepdims=True)
        l_send = jnp.sum(jnp.where(col == ch_send, logits, 0.0), axis=1, keepdims=True)
        top = jnp.maximum(l_keep, l_send)
        e_keep, e_send = jnp.exp(l_keep - top), jnp.exp(l_send - top)
        gate[...] = jnp.broadcast_to(e_keep / (e_keep + e_send), gate.shape)

    def unit(k):
        second[k].wait_recv()
        a = keep[k][0, mine] + rcv2[k][0].astype(F32)
        b = keep[k][1, mine] + rcv2[k][1].astype(F32)
        u_mine[k][mine] = (gate[mine][:, :1] * (a * jax.nn.sigmoid(a)) * b).astype(BF16)
        to_cross.extend(start_all([remote(u_mine[k].at[mine], u_mine[k].at[mine], s3.at[0, k], s3.at[1, k], x=cross)]))
        to_pair.extend(start_all([remote(u_mine[k].at[mine], u_pair[k].at[mine], s4.at[0, k], s4.at[1, k], x=pair)]))

    def pass_on(k):
        to_cross[k].wait_recv()
        forward.extend(start_all([remote(u_mine[k].at[other], u_pair[k].at[other], s5.at[0, k], s5.at[1, k], x=pair)]))

    def downward(k):
        lo, n = chunks[k]
        to_pair[k].wait_recv()
        forward[k].wait_recv()
        u0, u1 = u_mine[k][...], u_pair[k][...]
        total = jnp.zeros((rows, width), F32) if k == 0 else acc_down[...]
        for e in range(experts):
            total = total + dot_nt(u0 * wide_mask(0, e, n) + u1 * wide_mask(1, e, n), down[e, :, lo:lo + n])
        acc_down[...] = total

    sums(0)
    sums(1)
    gates()
    sums(2)
    for k in range(3, n_chunk):
        unit(k - 3)
        sums(k)
        if k > 3:
            pass_on(k - 4)
    for copy in loads[2 * experts:]:
        copy.wait()
    unit(n_chunk - 3)
    downward(0)
    unit(n_chunk - 2)
    pass_on(n_chunk - 4)
    for k in range(1, n_chunk - 3):
        downward(k)
    unit(n_chunk - 1)
    pass_on(n_chunk - 3)
    downward(n_chunk - 3)
    pass_on(n_chunk - 2)
    downward(n_chunk - 2)
    pass_on(n_chunk - 1)
    downward(n_chunk - 1)

    sums2, copies2 = [], []
    for i, (lo, n) in enumerate(halves):
        part2[i][...] = acc_down[:, lo:lo + n].astype(BF16)
        sums2.append(scatter_y(part2[i], rs2_in[i], rs2_sem.at[i], yi, y_count, span))
    for i, (lo, n) in enumerate(halves):
        for c in sums2[i]:
            c.wait()
        total = part2[i][own].astype(F32) + rs2_in[i][0].astype(F32) + rs2_in[i][1].astype(F32) + rs2_in[i][2].astype(F32)
        h_new = (x_mid[:, lo:lo + n].astype(F32) + total).astype(BF16)
        own2[i][...] = h_new
        copies2.append(gather_y(own2[i], all2[i], ag2_sem.at[i], yi, y_count, span))
        all2[i][own] = h_new
    for i, (lo, n) in enumerate(halves):
        for c in copies2[i]:
            c.wait()
        out_ref[:, lo:lo + n] = all2[i][...]
    for c in first + second + to_cross + to_pair + forward:
        c.wait_send()


def moe(mixed, w_o, x_own, gain, w_router, choice, w_act, w_lin, w_down, y_count, width_full):
    rows, heads = mixed.shape
    span, width = x_own.shape
    experts, _, ff = w_act.shape
    half, chunks = rows // 2, chunks_of(ff, 256)
    halves = ((0, 256), (256, width - 256))
    vmem, hbm = pl.BlockSpec(memory_space=pltpu.VMEM), pl.BlockSpec(memory_space=pl.ANY)
    down_t = jnp.transpose(w_down, (0, 2, 1))
    three = pltpu.SemaphoreType.DMA((2, 3))
    ring = pltpu.SemaphoreType.DMA((2, y_count - 1))
    per_chunk = pltpu.SemaphoreType.DMA((2, len(chunks)))
    buf = lambda lead, r, dt: [pltpu.VMEM(lead + (r, n), dt) for _, n in chunks]
    flat = (experts * width, ff)
    scratch = [pltpu.VMEM(flat, BF16), pltpu.VMEM(flat, BF16), pltpu.VMEM(down_t.shape, BF16), pltpu.VMEM((8, LANES), F32), pltpu.VMEM((3, 8, LANES), F32), pltpu.VMEM((rows, width), BF16), pltpu.VMEM((y_count - 1, span, width), BF16), pltpu.VMEM((span, width), BF16), pltpu.VMEM((rows, width), BF16), pltpu.VMEM((experts, 2 * LANES), F32), pltpu.VMEM((3, experts, 2 * LANES), F32), pltpu.VMEM((rows, LANES), F32), pltpu.VMEM((2, experts, rows, LANES), BF16), pltpu.VMEM((2, rows, experts * width), BF16), pltpu.VMEM((rows, width), F32), pltpu.VMEM((span, width), BF16), pltpu.VMEM(w_o.shape, BF16), pltpu.SemaphoreType.DMA]
    scratch += buf((2,), rows, F32) + buf((2,), rows, BF16) + buf((2,), rows, BF16) + buf((2,), half, BF16) + buf((2,), half, BF16) + buf((), rows, BF16) + buf((), rows, BF16)
    for lead, r in (((), rows), ((y_count - 1,), span), ((), span), ((), rows)):
        scratch += [pltpu.VMEM(lead + (r, n), BF16) for _, n in halves]
    rings = pltpu.SemaphoreType.DMA((2, 2, y_count - 1))
    scratch += [pltpu.SemaphoreType.DMA((3, experts)), three, ring, ring, three] + [per_chunk] * 5 + [rings, rings]
    return pl.pallas_call(
        functools.partial(moe_kernel, y_count, width_full, chunks, halves, experts),
        in_specs=[vmem, hbm] + [vmem] * 4 + [hbm] * 3,
        out_specs=vmem,
        out_shape=jax.ShapeDtypeStruct((rows, width), BF16),
        scratch_shapes=scratch,
        compiler_params=pltpu.CompilerParams(collective_id=1, has_side_effects=True, vmem_limit_bytes=67043328),
        cost_estimate=pl.CostEstimate(flops=2 * 10 ** 10, bytes_accessed=6 * w_act.size, transcendentals=0),
        name="moe",
    )(mixed, w_o, x_own, gain, w_router.T, choice, w_act, w_lin, down_t)


def rope_tables(lengths, steps, head):
    half = head // 2
    inv_freq = ROPE_BASE ** (-(jnp.arange(half, dtype=F32) * 2.0 / head))
    spots = (lengths[None, :] + jnp.arange(steps)[:, None]).reshape(-1).astype(F32)
    angles = spots[:, None] * inv_freq[None, :]
    return jnp.cos(angles), jnp.sin(angles)


def solution(mesh):
    x_count, y_count = mesh.shape['x'], mesh.shape['y']
    assert x_count == 4 and y_count == 4
    cache_spec = P('dp', None, 'y', None)
    in_specs = (P(None, 'dp'), P('dp'), P(None, 'dp', None), P(None, 'x'), cache_spec, cache_spec, P('x'), P('x', 'y'), P('x', 'y'), P('x', 'y'), P('y', 'x'), P('x'), P('x', None), P(None, 'x', 'y'), P(None, 'x', 'y'), P(None, 'y', 'x'))
    out_specs = (P(None, 'dp', 'x'), cache_spec, cache_spec)

    def per_device(tokens, lengths, choices, emb_table, k_cache, v_cache, g_attn, w_q, w_k, w_v, w_o, g_ffn, w_router, w_act, w_lin, w_down):
        steps, n_batch = tokens.shape
        heads, head = k_cache.shape[2], k_cache.shape[3]
        rows = steps * n_batch
        width_full = emb_table.shape[1] * x_count
        span = rows // y_count
        cos_t, sin_t = rope_tables(lengths, steps, head)
        x_own = gather(emb_table, tokens, span)
        kvq = qkv_sums(x_own, g_attn, w_q, w_k, w_v, rows, y_count, width_full)
        mixed, k_out, v_out = attention(lengths, kvq, cos_t, sin_t, k_cache, v_cache, steps)
        out = moe(mixed, w_o, x_own, g_ffn, w_router, jnp.transpose(choices, (0, 2, 1)), w_act, w_lin, w_down, y_count, width_full)
        return out.reshape(steps, n_batch, emb_table.shape[1]), k_out, v_out

    return jax.shard_map(per_device, mesh=mesh, in_specs=in_specs, out_specs=out_specs, check_vma=False)
```

```python
import functools
import jax
import jax.numpy as jnp
from jax import lax
from jax.experimental import pallas as pl
from jax.experimental.pallas import tpu as pltpu
from jax.sharding import PartitionSpec as P

EPS = 1e-5
ROPE_BASE = 1.0e6
F32 = jnp.float32
BF16 = jnp.bfloat16
LANES = 128


def dot(a, b):
    return lax.dot_general(a, b, (((1,), (0,)), ((), ())), preferred_element_type=F32)


def dot_nt(a, b):
    return lax.dot_general(a, b, (((1,), (1,)), ((), ())), preferred_element_type=F32)


def gather_kernel(span, vocab, depth, tok_ref, edge_ref, emb_ref, x_ref, buf, acc, sem):
    tiles = vocab // LANES
    batch = tok_ref.shape[1]
    start = lax.axis_index('y') * span

    def token(i):
        r = start + i
        return tok_ref[r // batch, lax.rem(r, batch)]

    def copy(i):
        tile = jnp.minimum(token(i) // LANES, tiles - 1)
        src = emb_ref.at[:, pl.ds(pl.multiple_of(tile * LANES, LANES), LANES)]
        slot = lax.rem(i, depth)
        return pltpu.make_async_copy(src, buf.at[slot], sem.at[slot])

    @pl.loop(0, min(depth, span))
    def _(i):
        copy(i).start()

    lane_id = lax.broadcasted_iota(jnp.int32, acc.shape, 1)

    @pl.loop(0, span)
    def _(i):
        copy(i).wait()
        tok = token(i)
        shift = lax.rem(i - lax.rem(tok, LANES) + LANES, LANES)
        edge = jnp.full(acc.shape, tok, jnp.int32) >= tiles * LANES
        moved = pltpu.roll(jnp.where(edge, edge_ref[...], buf[lax.rem(i, depth)]), shift, 1)
        acc[...] = jnp.where(lane_id == i, moved, acc[...])

        @pl.when(i + depth < span)
        def _():
            copy(i + depth).start()

    x_ref[...] = acc[...].astype(F32).T[:span].astype(BF16)


def gather(emb_table, tokens, span, depth=48):
    vocab, width = emb_table.shape
    table = emb_table.T
    return pl.pallas_call(
        functools.partial(gather_kernel, span, vocab, depth),
        grid=(1,),
        in_specs=[pl.BlockSpec(memory_space=pltpu.SMEM), pl.BlockSpec((width, LANES), lambda i: (0, vocab // LANES)), pl.BlockSpec(memory_space=pl.ANY)],
        out_specs=pl.BlockSpec((span, width), lambda i: (0, 0)),
        out_shape=jax.ShapeDtypeStruct((span, width), BF16),
        scratch_shapes=[pltpu.VMEM((depth, width, LANES), BF16), pltpu.VMEM((width, LANES), BF16), pltpu.SemaphoreType.DMA((depth,))],
        name="gather",
    )(tokens, table, table)


def attention_kernel(steps, batch, block, heads, head, lens_ref, kvq_ref, cos_ref, sin_ref, k_in, v_in, o_ref, k_out, v_out, q_rows, kt_ref, vt_ref, o_rows):
    cols = heads * head
    slots = k_in.shape[-1]
    rows = steps * batch
    i = pl.program_id(0)
    hpad = 16
    per_group = slots // 4

    @pl.when(i == 0)
    def _():
        def spread(table):
            four = jnp.concatenate([table] * (LANES // table.shape[1]), axis=1)
            return jnp.concatenate([four] * (cols // LANES) + [four[:, :cols % LANES]], axis=1)

        cosine, sine = spread(cos_ref[...]), spread(sin_ref[...])
        src = lax.broadcasted_iota(jnp.int32, (cols, cols), 0)
        dst = lax.broadcasted_iota(jnp.int32, (cols, cols), 1)
        low = dst % head < head // 2
        swap = jnp.where(low & (src == dst + head // 2), -1.0, jnp.where(~low & (src == dst - head // 2), 1.0, 0.0)).astype(BF16)
        row = lax.broadcasted_iota(jnp.int32, (rows, 4 * batch), 0)
        col = lax.broadcasted_iota(jnp.int32, (rows, 4 * batch), 1)
        perm = jnp.where((row // batch == col % 4) & (row % batch == col // 4), 1.0, 0.0).astype(BF16)
        for part in (2, 0):
            val = kvq_ref[part]
            swapped = dot(val, swap)
            rot = (val.astype(F32) * cosine + swapped * sine).astype(BF16).astype(F32)
            if part == 2:
                q_rows[...] = rot.reshape(steps, batch, cols)
            else:
                kt = dot(rot.T.astype(BF16), perm)
        vt = dot(kvq_ref[1].astype(F32).T.astype(BF16), perm)
        for g in range(batch // per_group):
            kt_ref[g] = kt[:, g * slots:(g + 1) * slots].astype(kt_ref.dtype)
            vt_ref[g] = vt[:, g * slots:(g + 1) * slots].astype(vt_ref.dtype)

    head_mask = lax.broadcasted_iota(jnp.int32, (hpad, cols), 1) // head == lax.broadcasted_iota(jnp.int32, (hpad, cols), 0)
    t_of = lax.broadcasted_iota(jnp.int32, (steps * hpad, slots), 0) // hpad
    s_of = lax.broadcasted_iota(jnp.int32, (steps * hpad, slots), 1)
    slot_id = lax.broadcasted_iota(jnp.int32, (cols, slots), 1)

    group = (i * block) // per_group
    news, scores_all = [], []
    for n in range(block):
        b = i * block + n
        first = lens_ref[b]
        shift = lax.rem(first - 4 * lax.rem(b, per_group) + slots, slots)
        fresh = (slot_id >= first) & (slot_id < first + steps)
        k_new = jnp.where(fresh, pltpu.roll(kt_ref[group], shift, 1).astype(BF16), k_in[n].reshape(cols, slots))
        v_new = jnp.where(fresh, pltpu.roll(vt_ref[group], shift, 1).astype(BF16), v_in[n].reshape(cols, slots))
        k_out[n] = k_new.reshape(heads, head, slots)
        v_out[n] = v_new.reshape(heads, head, slots)
        q_blk = jnp.concatenate([jnp.where(head_mask, jnp.broadcast_to(q_rows[t, pl.ds(b, 1), :], (hpad, cols)), 0.0) for t in range(steps)], axis=0).astype(BF16)
        scores = dot(q_blk, k_new) * head ** -0.5
        scores_all.append(jnp.where(s_of <= first + t_of, scores, -1.0e30))
        news.append(v_new)
    scores = jnp.concatenate(scores_all, axis=0)
    peak = jnp.max(scores, axis=-1, keepdims=True)
    weight = jnp.exp(scores - peak)
    inverse = 1.0 / jnp.sum(weight, axis=-1, keepdims=True)
    weight = weight.astype(BF16)
    span = steps * hpad
    for n in range(block):
        b = i * block + n
        mixed = dot_nt(weight[n * span:(n + 1) * span], news[n]) * inverse[n * span:(n + 1) * span]
        for t in range(steps):
            o_rows[t, pl.ds(b, 1), :] = jnp.sum(jnp.where(head_mask, mixed[t * hpad:(t + 1) * hpad], 0.0), axis=0, keepdims=True)

    @pl.when(i == pl.num_programs(0) - 1)
    def _():
        o_ref[...] = o_rows[...].reshape(rows, cols).astype(BF16)


def attention(lengths, kvq, cos_t, sin_t, k_cache, v_cache, steps, block=16, roll_dtype=BF16):
    batch, slots, heads, head = k_cache.shape
    cols, rows = heads * head, steps * batch
    k_t, v_t = jnp.transpose(k_cache, (0, 2, 3, 1)), jnp.transpose(v_cache, (0, 2, 3, 1))
    whole = lambda shape: pl.BlockSpec(shape, lambda i: (0,) * len(shape))
    cache_blk = pl.BlockSpec((block, heads, head, slots), lambda i: (i, 0, 0, 0))
    groups = 4 * batch // slots
    o, k_o, v_o = pl.pallas_call(
        functools.partial(attention_kernel, steps, batch, block, heads, head),
        grid=(batch // block,),
        in_specs=[pl.BlockSpec(memory_space=pltpu.SMEM), whole((3, rows, cols)), whole((rows, head // 2)), whole((rows, head // 2)), cache_blk, cache_blk],
        out_specs=[whole((rows, cols)), cache_blk, cache_blk],
        out_shape=[jax.ShapeDtypeStruct((rows, cols), BF16), jax.ShapeDtypeStruct(k_t.shape, BF16), jax.ShapeDtypeStruct(v_t.shape, BF16)],
        scratch_shapes=[pltpu.VMEM((steps, batch, cols), F32), pltpu.VMEM((groups, cols, slots), roll_dtype), pltpu.VMEM((groups, cols, slots), roll_dtype), pltpu.VMEM((steps, batch, cols), F32)],
        compiler_params=pltpu.CompilerParams(dimension_semantics=("arbitrary",)),
        cost_estimate=pl.CostEstimate(flops=4 * 10 ** 9, bytes_accessed=4 * k_t.size * 2, transcendentals=0),
        name="attention",
    )(lengths, kvq, cos_t, sin_t, k_t, v_t)
    back = lambda a: jnp.transpose(a, (0, 3, 1, 2))
    return o, back(k_o), back(v_o)


X, Y = 'x', 'y'
MESH = pl.DeviceIdType.MESH


def positions():
    xi, yi = lax.axis_index(X), lax.axis_index(Y)
    core, chip = lax.rem(xi, 2), xi // 2
    pair = xi + 1 - 2 * core
    cross = lax.rem(xi + 2, 4)
    diag = lax.rem(pair + 2, 4)
    return xi, yi, core, chip, pair, cross, diag


def knock(x_peers, yi, y_count):
    barrier = pltpu.get_barrier_semaphore()
    for peer in x_peers:
        pl.semaphore_signal(barrier, inc=1, device_id={X: peer}, device_id_type=MESH)
    for d in range(1, y_count):
        pl.semaphore_signal(barrier, inc=1, device_id={Y: lax.rem(yi + d, y_count)}, device_id_type=MESH)
    return lambda: pl.semaphore_wait(barrier, len(x_peers) + y_count - 1)


def remote(src, dst, send, recv, **where):
    return pltpu.make_async_remote_copy(src_ref=src, dst_ref=dst, send_sem=send, recv_sem=recv, device_id=where, device_id_type=MESH)


def start_all(copies):
    for c in copies:
        c.start()
    return copies


def scatter_y(src, dst, sems, yi, y_count, span):
    out = []
    for d in range(1, y_count):
        peer = lax.rem(yi + d, y_count)
        rows = pl.ds(pl.multiple_of(peer * span, span), span)
        out.append(remote(src.at[rows], dst.at[d - 1], sems.at[0, d - 1], sems.at[1, d - 1], y=peer))
    return start_all(out)


def gather_y(src, dst, sems, yi, y_count, span):
    rows = pl.ds(pl.multiple_of(yi * span, span), span)
    return start_all([remote(src, dst.at[rows], sems.at[0, d - 1], sems.at[1, d - 1], y=lax.rem(yi + d, y_count)) for d in range(1, y_count)])


def normalise(x_f32, gain, stat, stat_in, sems, peers, width_full, ready=None):
    rows = x_f32.shape[0]
    part = jnp.sum(x_f32 * x_f32, axis=-1, keepdims=True)
    stat[:, :rows] = jnp.broadcast_to(part, (rows, LANES)).T[:8]
    if ready:
        ready()
    copies = start_all([remote(stat, stat_in.at[i], sems.at[0, i], sems.at[1, i], x=peer) for i, peer in enumerate(peers)])
    for c in copies:
        c.wait()
    total = ((stat[...] + stat_in[0]) + (stat_in[1] + stat_in[2])).T[:rows, :1]
    return (x_f32 * lax.rsqrt(total / width_full + EPS) * gain).astype(BF16)


def qkv_kernel(y_count, width_full, x_ref, g_ref, wk_hbm, wv_hbm, wq_hbm, out_ref, weights, w_sem, stat, stat_in, h_own, h_all, keep, snd1, rcv1, snd2, rcv2, done, rcv3, stat_sem, y_sem, s1, s2, s3):
    xi, yi, core, chip, pair, cross, diag = positions()
    span, rows = x_ref.shape[0], h_all.shape[0]
    half = rows // 2
    ready = knock((pair, cross, diag), yi, y_count)
    loads = start_all([pltpu.make_async_copy(w, weights.at[m], w_sem.at[m]) for m, w in enumerate((wk_hbm, wv_hbm, wq_hbm))])
    stat[...] = jnp.zeros_like(stat)
    h = normalise(x_ref[...].astype(F32), g_ref[...].astype(F32)[None, :], stat, stat_in, stat_sem, (pair, cross, diag), width_full, ready)
    h_own[...] = h
    sent = gather_y(h_own, h_all, y_sem, yi, y_count, span)
    h_all[pl.ds(pl.multiple_of(yi * span, span), span)] = h
    for c in sent:
        c.wait()
    mine = pl.ds(pl.multiple_of(core * half, half), half)
    theirs = pl.ds(pl.multiple_of((1 - core) * half, half), half)
    first, second, third = [], [], []
    for m in range(3):
        loads[m].wait()
        snd1[m] = dot(h_all[theirs], weights[m]).astype(BF16)
        first += start_all([remote(snd1.at[m], rcv1.at[m], s1.at[0, m], s1.at[1, m], x=pair)])
        keep[m] = dot(h_all[mine], weights[m])
        first[m].wait_recv()
        snd2[m] = (keep[m] + rcv1[m].astype(F32)).astype(BF16)
        second += start_all([remote(snd2.at[m], rcv2.at[m], s2.at[0, m], s2.at[1, m], x=cross)])
    for m in range(3):
        second[m].wait_recv()
        done[m] = (snd2[m].astype(F32) + rcv2[m].astype(F32)).astype(BF16)
        third += start_all([remote(done.at[m], rcv3.at[m], s3.at[0, m], s3.at[1, m], x=pair)])
        out_ref[m, mine] = done[m]
    for m in range(3):
        third[m].wait_recv()
        out_ref[m, theirs] = rcv3[m]
    for c in first + second + third:
        c.wait_send()


def qkv_sums(x_own, gain, w_q, w_k, w_v, rows, y_count, width_full):
    span, width = x_own.shape
    cols, half = w_q.shape[1], rows // 2
    vmem = pl.BlockSpec(memory_space=pltpu.VMEM)
    part = pltpu.VMEM((3, half, cols), BF16)
    pairs = pltpu.SemaphoreType.DMA((2, 3))
    return pl.pallas_call(
        functools.partial(qkv_kernel, y_count, width_full),
        in_specs=[vmem] * 2 + [pl.BlockSpec(memory_space=pl.ANY)] * 3,
        out_specs=vmem,
        out_shape=jax.ShapeDtypeStruct((3, rows, cols), BF16),
        scratch_shapes=[pltpu.VMEM((3, width, cols), BF16), pltpu.SemaphoreType.DMA((3,)), pltpu.VMEM((8, LANES), F32), pltpu.VMEM((3, 8, LANES), F32), pltpu.VMEM((span, width), BF16), pltpu.VMEM((rows, width), BF16), pltpu.VMEM((3, half, cols), F32), part, part, part, part, part, part, pairs, pltpu.SemaphoreType.DMA((2, y_count - 1)), pairs, pairs, pairs],
        compiler_params=pltpu.CompilerParams(collective_id=0, has_side_effects=True),
        cost_estimate=pl.CostEstimate(flops=6 * rows * width * cols, bytes_accessed=8 * width * cols, transcendentals=0),
        name="qkv_sums",
    )(x_own, gain, w_k, w_v, w_q)


def chunks_of(ff, wide):
    return tuple((lo, min(wide, ff - lo)) for lo in range(0, ff, wide))


def moe_kernel(y_count, width_full, chunks, halves, experts, o_ref, wo_hbm, x_ref, g_ref, wr_ref, ch_ref, act_hbm, lin_hbm, down_hbm, out_ref, act, lin, down, stat, stat_in, part, rs_in, h_own, h_all, logit, logit_in, gate, mask, sparse, acc_down, x_mid, wo, wo_sem, *rest):
    n_chunk = len(chunks)
    keep, snd1, rcv1, snd2, rcv2, u_mine, u_pair = [rest[i * n_chunk:(i + 1) * n_chunk] for i in range(7)]
    last = rest[7 * n_chunk:7 * n_chunk + 8]
    part2, rs2_in, own2, all2 = last[:2], last[2:4], last[4:6], last[6:]
    w_sem, stat_sem, rs_sem, ag_sem, lg_sem, s1, s2, s3, s4, s5, rs2_sem, ag2_sem = rest[7 * n_chunk + 8:]
    xi, yi, core, chip, pair, cross, diag = positions()
    peers = (pair, cross, diag)
    span, rows = x_ref.shape[0], h_all.shape[0]
    half, width = rows // 2, x_ref.shape[1]
    ready = knock(peers, yi, y_count)
    wo_load = pltpu.make_async_copy(wo_hbm, wo, wo_sem)
    wo_load.start()
    loads = []
    for i, (src, dst) in enumerate(((act_hbm, act), (lin_hbm, lin), (down_hbm, down))):
        for e in range(experts):
            place = dst.at[e] if i == 2 else dst.at[pl.ds(e * width, width)]
            loads.append(pltpu.make_async_copy(src.at[e], place, w_sem.at[i, e]))
    stat[...] = jnp.zeros_like(stat)
    logit[...] = jnp.zeros_like(logit)
    own = pl.ds(pl.multiple_of(yi * span, span), span)
    wo_load.wait()
    start_all(loads)
    part[...] = dot(o_ref[...], wo[...]).astype(BF16)
    ch = ch_ref[...].astype(F32)
    ch = jnp.concatenate([jnp.concatenate([ch[t], jnp.zeros((8 - ch.shape[1], ch.shape[2]), F32)], axis=0).T for t in range(ch.shape[0])], axis=0)
    ch_keep = jnp.where(core == 0, ch[:, :1], ch[:, 1:2])
    ch_send = jnp.where(core == 0, ch[:, 1:2], ch[:, :1])
    for e in range(experts):
        mask[0, e] = jnp.broadcast_to(jnp.where(ch_keep == e, 1.0, 0.0), (rows, LANES)).astype(BF16)
        mask[1, e] = jnp.broadcast_to(jnp.where(ch_send == e, 1.0, 0.0), (rows, LANES)).astype(BF16)

    ready()
    sent = scatter_y(part, rs_in, rs_sem, yi, y_count, span)

    def wide_mask(s, e, n):
        return jnp.concatenate([mask[s, e]] * (n // LANES) + ([mask[s, e][:, :n % LANES]] if n % LANES else []), axis=1)

    for c in sent:
        c.wait()
    total = part[own].astype(F32) + rs_in[0].astype(F32) + rs_in[1].astype(F32) + rs_in[2].astype(F32)
    x_new = (x_ref[...].astype(F32) + total).astype(BF16)
    x_mid[...] = x_new
    h = normalise(x_new.astype(F32), g_ref[...].astype(F32)[None, :], stat, stat_in, stat_sem, peers, width_full)
    h_own[...] = h
    sent = gather_y(h_own, h_all, ag_sem, yi, y_count, span)
    h_all[own] = h
    for c in sent:
        c.wait()
    logit[:, :rows] = dot_nt(wr_ref[...], h_all[...])
    lg = start_all([remote(logit, logit_in.at[i], lg_sem.at[0, i], lg_sem.at[1, i], x=peer) for i, peer in enumerate(peers)])
    h2 = h_all[...]
    for e in range(experts):
        for s in range(2):
            sparse[s, :, e * width:(e + 1) * width] = h2 * wide_mask(s, e, width)

    for copy in loads[:2 * experts]:
        copy.wait()

    mine = pl.ds(pl.multiple_of(chip * half, half), half)
    other = pl.ds(pl.multiple_of((1 - chip) * half, half), half)
    first, second, to_cross, to_pair, forward = [], [], [], [], []

    def product(s, w, lo, n):
        return dot(sparse[s], w[:, lo:lo + n])

    def sums(k):
        lo, n = chunks[k]
        snd1[k][0] = product(1, act, lo, n).astype(BF16)
        snd1[k][1] = product(1, lin, lo, n).astype(BF16)
        first.extend(start_all([remote(snd1[k], rcv1[k], s1.at[0, k], s1.at[1, k], x=pair)]))
        keep[k][0] = product(0, act, lo, n)
        keep[k][1] = product(0, lin, lo, n)
        first[k].wait_recv()
        for i in range(2):
            snd2[k][i] = (keep[k][i, other] + rcv1[k][i, other].astype(F32)).astype(BF16)
        second.extend(start_all([remote(snd2[k], rcv2[k], s2.at[0, k], s2.at[1, k], x=cross)]))
        for i in range(2):
            keep[k][i, mine] = keep[k][i, mine] + rcv1[k][i, mine].astype(F32)

    def gates():
        for c in lg:
            c.wait()
        logits = ((logit[...] + logit_in[0]) + (logit_in[1] + logit_in[2])).T[:rows]
        col = lax.broadcasted_iota(jnp.int32, logits.shape, 1).astype(F32)
        l_keep = jnp.sum(jnp.where(col == ch_keep, logits, 0.0), axis=1, keepdims=True)
        l_send = jnp.sum(jnp.where(col == ch_send, logits, 0.0), axis=1, keepdims=True)
        top = jnp.maximum(l_keep, l_send)
        e_keep, e_send = jnp.exp(l_keep - top), jnp.exp(l_send - top)
        gate[...] = jnp.broadcast_to(e_keep / (e_keep + e_send), gate.shape)

    def unit(k):
        second[k].wait_recv()
        a = keep[k][0, mine] + rcv2[k][0].astype(F32)
        b = keep[k][1, mine] + rcv2[k][1].astype(F32)
        u_mine[k][mine] = (gate[mine][:, :1] * (a * jax.nn.sigmoid(a)) * b).astype(BF16)
        to_cross.extend(start_all([remote(u_mine[k].at[mine], u_mine[k].at[mine], s3.at[0, k], s3.at[1, k], x=cross)]))
        to_pair.extend(start_all([remote(u_mine[k].at[mine], u_pair[k].at[mine], s4.at[0, k], s4.at[1, k], x=pair)]))

    def pass_on(k):
        to_cross[k].wait_recv()
        forward.extend(start_all([remote(u_mine[k].at[other], u_pair[k].at[other], s5.at[0, k], s5.at[1, k], x=pair)]))

    def downward(k):
        lo, n = chunks[k]
        to_pair[k].wait_recv()
        forward[k].wait_recv()
        u0, u1 = u_mine[k][...], u_pair[k][...]
        total = jnp.zeros((width, rows), F32) if k == 0 else acc_down[...]
        for e in range(experts):
            total = total + dot_nt(down[e, :, lo:lo + n], u0 * wide_mask(0, e, n) + u1 * wide_mask(1, e, n))
        acc_down[...] = total

    sums(0)
    sums(1)
    gates()
    sums(2)
    for k in range(3, n_chunk):
        unit(k - 3)
        sums(k)
        if k > 3:
            pass_on(k - 4)
    for copy in loads[2 * experts:]:
        copy.wait()
    unit(n_chunk - 3)
    downward(0)
    unit(n_chunk - 2)
    pass_on(n_chunk - 4)
    for k in range(1, n_chunk - 3):
        downward(k)
    unit(n_chunk - 1)
    pass_on(n_chunk - 3)
    downward(n_chunk - 3)
    pass_on(n_chunk - 2)
    downward(n_chunk - 2)
    pass_on(n_chunk - 1)
    downward(n_chunk - 1)

    sums2, copies2 = [], []
    for i, (lo, n) in enumerate(halves):
        part2[i][...] = acc_down[lo:lo + n].T.astype(BF16)
        sums2.append(scatter_y(part2[i], rs2_in[i], rs2_sem.at[i], yi, y_count, span))
    for i, (lo, n) in enumerate(halves):
        for c in sums2[i]:
            c.wait()
        total = part2[i][own].astype(F32) + rs2_in[i][0].astype(F32) + rs2_in[i][1].astype(F32) + rs2_in[i][2].astype(F32)
        h_new = (x_mid[:, lo:lo + n].astype(F32) + total).astype(BF16)
        own2[i][...] = h_new
        copies2.append(gather_y(own2[i], all2[i], ag2_sem.at[i], yi, y_count, span))
        all2[i][own] = h_new
    for i, (lo, n) in enumerate(halves):
        for c in copies2[i]:
            c.wait()
        out_ref[:, lo:lo + n] = all2[i][...]
    for c in first + second + to_cross + to_pair + forward:
        c.wait_send()


def moe(mixed, w_o, x_own, gain, w_router, choice, w_act, w_lin, w_down, y_count, width_full):
    rows, heads = mixed.shape
    span, width = x_own.shape
    experts, _, ff = w_act.shape
    half, chunks = rows // 2, chunks_of(ff, 256)
    halves = ((0, 256), (256, width - 256))
    vmem, hbm = pl.BlockSpec(memory_space=pltpu.VMEM), pl.BlockSpec(memory_space=pl.ANY)
    down_t = jnp.transpose(w_down, (0, 2, 1))
    three = pltpu.SemaphoreType.DMA((2, 3))
    ring = pltpu.SemaphoreType.DMA((2, y_count - 1))
    per_chunk = pltpu.SemaphoreType.DMA((2, len(chunks)))
    buf = lambda lead, r, dt: [pltpu.VMEM(lead + (r, n), dt) for _, n in chunks]
    flat = (experts * width, ff)
    scratch = [pltpu.VMEM(flat, BF16), pltpu.VMEM(flat, BF16), pltpu.VMEM(down_t.shape, BF16), pltpu.VMEM((8, LANES), F32), pltpu.VMEM((3, 8, LANES), F32), pltpu.VMEM((rows, width), BF16), pltpu.VMEM((y_count - 1, span, width), BF16), pltpu.VMEM((span, width), BF16), pltpu.VMEM((rows, width), BF16), pltpu.VMEM((experts, 2 * LANES), F32), pltpu.VMEM((3, experts, 2 * LANES), F32), pltpu.VMEM((rows, LANES), F32), pltpu.VMEM((2, experts, rows, LANES), BF16), pltpu.VMEM((2, rows, experts * width), BF16), pltpu.VMEM((width, rows), F32), pltpu.VMEM((span, width), BF16), pltpu.VMEM(w_o.shape, BF16), pltpu.SemaphoreType.DMA]
    scratch += buf((2,), rows, F32) + buf((2,), rows, BF16) + buf((2,), rows, BF16) + buf((2,), half, BF16) + buf((2,), half, BF16) + buf((), rows, BF16) + buf((), rows, BF16)
    for lead, r in (((), rows), ((y_count - 1,), span), ((), span), ((), rows)):
        scratch += [pltpu.VMEM(lead + (r, n), BF16) for _, n in halves]
    rings = pltpu.SemaphoreType.DMA((2, 2, y_count - 1))
    scratch += [pltpu.SemaphoreType.DMA((3, experts)), three, ring, ring, three] + [per_chunk] * 5 + [rings, rings]
    return pl.pallas_call(
        functools.partial(moe_kernel, y_count, width_full, chunks, halves, experts),
        in_specs=[vmem, hbm] + [vmem] * 4 + [hbm] * 3,
        out_specs=vmem,
        out_shape=jax.ShapeDtypeStruct((rows, width), BF16),
        scratch_shapes=scratch,
        compiler_params=pltpu.CompilerParams(collective_id=1, has_side_effects=True, vmem_limit_bytes=67043328),
        cost_estimate=pl.CostEstimate(flops=2 * 10 ** 10, bytes_accessed=6 * w_act.size, transcendentals=0),
        name="moe",
    )(mixed, w_o, x_own, gain, w_router.T, choice, w_act, w_lin, down_t)


def rope_tables(lengths, steps, head):
    half = head // 2
    inv_freq = ROPE_BASE ** (-(jnp.arange(half, dtype=F32) * 2.0 / head))
    spots = (lengths[None, :] + jnp.arange(steps)[:, None]).reshape(-1).astype(F32)
    angles = spots[:, None] * inv_freq[None, :]
    return jnp.cos(angles), jnp.sin(angles)


def solution(mesh):
    x_count, y_count = mesh.shape['x'], mesh.shape['y']
    assert x_count == 4 and y_count == 4
    cache_spec = P('dp', None, 'y', None)
    in_specs = (P(None, 'dp'), P('dp'), P(None, 'dp', None), P(None, 'x'), cache_spec, cache_spec, P('x'), P('x', 'y'), P('x', 'y'), P('x', 'y'), P('y', 'x'), P('x'), P('x', None), P(None, 'x', 'y'), P(None, 'x', 'y'), P(None, 'y', 'x'))
    out_specs = (P(None, 'dp', 'x'), cache_spec, cache_spec)

    def per_device(tokens, lengths, choices, emb_table, k_cache, v_cache, g_attn, w_q, w_k, w_v, w_o, g_ffn, w_router, w_act, w_lin, w_down):
        steps, n_batch = tokens.shape
        heads, head = k_cache.shape[2], k_cache.shape[3]
        rows = steps * n_batch
        width_full = emb_table.shape[1] * x_count
        span = rows // y_count
        cos_t, sin_t = rope_tables(lengths, steps, head)
        x_own = gather(emb_table, tokens, span)
        kvq = qkv_sums(x_own, g_attn, w_q, w_k, w_v, rows, y_count, width_full)
        mixed, k_out, v_out = attention(lengths, kvq, cos_t, sin_t, k_cache, v_cache, steps)
        out = moe(mixed, w_o, x_own, g_ffn, w_router, jnp.transpose(choices, (0, 2, 1)), w_act, w_lin, w_down, y_count, width_full)
        return out.reshape(steps, n_batch, emb_table.shape[1]), k_out, v_out

    return jax.shard_map(per_device, mesh=mesh, in_specs=in_specs, out_specs=out_specs, check_vma=False)
```
